32 devices in a mesh: tm: 16 (over z, y, core), series: 2 (over x).
Axes of the slice: x: 2, y: 2, z: 4, core: 2. Of those that a mesh axis runs over, the one named last changes fastest.
Arguments:
- history: bfloat16 [4, 4096, 1024], P('series', 'tm'), may hold values from -36 to 36
- lengths: int32 [4], P('series'), may hold values from 512 to 4096
- head_window: int32 [16], replicated, may hold values from 32 to 512, as said below
- input_proj: bfloat16 [1024, 3072], replicated
- output_proj: bfloat16 [1024, 1024], replicated, may hold values from -0.1875 to 0.1875
- mixer_down: bfloat16 [1024, 512], replicated, may hold values from -0.1875 to 0.1875
- mixer_up: bfloat16 [512, 1024], replicated, may hold values from -0.25 to 0.25
- series_mix: bfloat16 [4, 4], replicated, may hold values from -3 to 3
Outputs:
- layer_out: bfloat16 [4, 4096, 1024], P('series', 'tm')
The draws below stay inside these ranges and needn't reach their ends.
Inputs may be any that keep to these rules, and one draw needn't show every extreme that they name: `head_window`: some head has exactly 512.
All inputs are finite; a program needn't handle non-finite values.
Results may differ from the reference program's by a relative error of at most 0.0065.
Values may be sent and summed in bfloat16 or wider, within the bound.
No kernel may reach another device: no remote copies, remote signals or barrier semaphores. Data moves between devices by JAX's collectives and lax.ppermute only.
A program may use at most 128 MiB of HBM per device.

```python
import jax
import jax.numpy as jnp
from jax import lax

D = 1024
HEADS = 16
MIX_WIDTH = 512
WINDOW = 512
PATCHES = 4096
SERIES = 4


def draw_history(key, part):
    base = jnp.clip(jax.random.normal(key, (SERIES, PATCHES, D), jnp.float32), -6.0, 6.0)
    return base.astype(jnp.bfloat16)


def draw_head_window(key, part):
    windows = jax.random.randint(key, (HEADS,), max(WINDOW // 16, 1), WINDOW + 1, dtype=jnp.int32)
    chosen = jax.random.randint(jax.random.fold_in(key, 7), (), 0, HEADS, dtype=jnp.int32)
    return windows.at[chosen].set(WINDOW)


def draw_input_proj(key, part):
    first = jax.random.normal(jax.random.fold_in(key, 1), (D, D), jnp.float32)
    second = jax.random.normal(jax.random.fold_in(key, 2), (D, D), jnp.float32)
    third = jax.random.normal(jax.random.fold_in(key, 3), (D, D), jnp.float32)
    keyed = 0.6 * first + 0.8 * second
    return (jnp.concatenate([first, keyed, third], axis=1) * D ** (-0.5)).astype(jnp.bfloat16)


def with_ends(result, own_key, smallest, high):
    longest = result.shape.index(max(result.shape))
    spots = []
    for shift in (0, 1):
        where = [jax.random.randint(jax.random.fold_in(own_key, axis), (), 0, length) for axis, length in enumerate(result.shape)]
        where[longest] = (where[longest] + shift) % result.shape[longest]
        spots.append(tuple(where))
    return result.at[spots[0]].set(smallest).at[spots[1]].set(high)


def normal_values(key, shape, deviation, limit, kind=jnp.bfloat16):
    result = deviation * jax.random.normal(key, shape, jnp.float32)
    return jnp.clip(result, min=-limit, max=limit).astype(kind)


def setup_inputs(seed: int = 0) -> dict:
    key_list = jax.random.split(jax.random.key(seed), 9)
    return {
        "history": draw_history(jax.random.fold_in(key_list[8], 71), 0),
        "lengths": with_ends(jax.random.randint(key_list[1], (SERIES,), WINDOW, PATCHES + 1), jax.random.fold_in(key_list[1], 1), WINDOW, PATCHES).astype(jnp.int32),
        "head_window": draw_head_window(jax.random.fold_in(key_list[8], 71), 0),
        "input_proj": draw_input_proj(jax.random.fold_in(key_list[8], 71), 0),
        "output_proj": normal_values(key_list[4], (D, D), D ** -0.5, 0.1875),
        "mixer_down": normal_values(key_list[5], (D, MIX_WIDTH), D ** -0.5, 0.1875),
        "mixer_up": normal_values(key_list[6], (MIX_WIDTH, D), MIX_WIDTH ** -0.5, 0.25),
        "series_mix": normal_values(key_list[7], (SERIES, SERIES), SERIES ** -0.5, 3.0),
    }


def attend(queries, keys_values, length, head_window, query_first, key_first):
    query_rows = queries.shape[0]
    key_rows = keys_values.shape[0]
    head_size = D // HEADS
    query_heads = queries.astype(jnp.float32).reshape(query_rows, HEADS, head_size)
    key_heads = keys_values[:, :D].astype(jnp.float32).reshape(key_rows, HEADS, head_size)
    value_heads = keys_values[:, D:].astype(jnp.float32).reshape(key_rows, HEADS, head_size)
    scores = jnp.einsum("qhd,khd->hqk", query_heads, key_heads) * (head_size ** -0.5)
    query_pos = query_first + jnp.arange(query_rows, dtype=jnp.int32)
    key_pos = key_first + jnp.arange(key_rows, dtype=jnp.int32)
    key_valid = (key_pos >= PATCHES - length) & (key_pos < PATCHES)
    distance = jnp.abs(query_pos[:, None] - key_pos[None, :])
    allowed = (distance[None, :, :] <= head_window[:, None, None]) & key_valid[None, None, :]
    scores = jnp.where(allowed, scores, -1e30)
    largest = jnp.max(scores, axis=-1, keepdims=True)
    weights = jnp.exp(scores - largest)
    totals = jnp.sum(weights, axis=-1)
    probabilities = weights.astype(jnp.bfloat16).astype(jnp.float32)
    combined = jnp.einsum("hqk,khd->qhd", probabilities, value_heads) / jnp.transpose(totals)[:, :, None]
    combined = combined.reshape(query_rows, D)
    query_valid = query_pos >= PATCHES - length
    return jnp.where(query_valid[:, None], combined, 0.0).astype(jnp.bfloat16)


def reference(history, lengths, head_window, input_proj, output_proj, mixer_down, mixer_up, series_mix):
    block_rows = min(512, PATCHES)
    block_count = PATCHES // block_rows

    def per_series(inputs):
        series_rows, length = inputs
        packed = jnp.dot(series_rows, input_proj, preferred_element_type=jnp.float32).astype(jnp.bfloat16)
        queries = packed[:, :D]
        padded = jnp.pad(packed[:, D:], ((WINDOW, WINDOW), (0, 0)))

        def per_block(block_index):
            first_row = (block_index * block_rows).astype(jnp.int32)
            query_block = lax.dynamic_slice_in_dim(queries, first_row, block_rows, 0)
            key_block = lax.dynamic_slice_in_dim(padded, first_row, block_rows + 2 * WINDOW, 0)
            return attend(query_block, key_block, length, head_window, first_row, first_row - WINDOW)

        attended = lax.map(per_block, jnp.arange(block_count, dtype=jnp.int32)).reshape(PATCHES, D)
        hidden = (series_rows.astype(jnp.float32) + jnp.dot(attended, output_proj, preferred_element_type=jnp.float32)).astype(jnp.bfloat16)
        branch = jnp.dot(hidden, mixer_down, preferred_element_type=jnp.float32).astype(jnp.bfloat16)
        return hidden, branch

    hidden, branch = lax.map(per_series, (history, lengths))
    combined = jnp.einsum("ab,bpc->apc", series_mix.astype(jnp.float32), branch.astype(jnp.float32)).astype(jnp.bfloat16)
    update = jnp.dot(combined.reshape(SERIES * PATCHES, MIX_WIDTH), mixer_up, preferred_element_type=jnp.float32)
    return (hidden.astype(jnp.float32) + update.reshape(SERIES, PATCHES, D)).astype(jnp.bfloat16)
```

```python
import math

import jax
import jax.numpy as jnp
from jax import lax
from jax.experimental import pallas as pl
from jax.experimental.pallas import tpu as pltpu
from jax.sharding import PartitionSpec as P

HEADS = 16
WINDOW = 512
LANES = 128
MASKED = -1e30


def routes(count):
    place = lambda quad, chip, core: 4 * quad + 2 * chip + core
    last = count // 4 - 1
    chip_swap = [(i, i ^ 2) for i in range(count)]
    core_swap = [(i, i ^ 1) for i in range(count)]
    near, far = [], []
    for i in range(count):
        quad, chip, core = i // 4, (i // 2) % 2, i % 2
        down = quad - 1 if quad > 0 else None
        up = quad + 1 if quad < last else None
        near_quad, far_quad = (down, up) if chip == 0 else (up, down)
        if near_quad is not None:
            near.append((i, place(near_quad, chip, core)))
        if far_quad is not None:
            far.append((i, place(far_quad, chip, core)))
    return chip_swap, core_swap, near, far


def project(pieces, slots, weight, first_column, slot_count, buffer=None):
    rows, width = pieces[0].shape
    columns = weight.shape[1] - first_column
    chunk = min(512, columns)
    count = len(pieces)

    def body(slots_ref, *refs):
        piece_refs = refs[:count]
        weight_ref = refs[count]
        out_ref = refs[-1]
        for index in range(count):

            @pl.when(pl.program_id(1) == index)
            def _():
                out_ref[0] = jnp.dot(
                    piece_refs[index][...], weight_ref[...], preferred_element_type=jnp.float32
                ).astype(out_ref.dtype)

    in_specs = [pl.BlockSpec((rows, width), lambda j, i, s: (0, 0)) for _ in pieces]
    in_specs.append(
        pl.BlockSpec((width, chunk), lambda j, i, s: (0, first_column // chunk + j))
    )
    operands = list(pieces) + [weight]
    aliases = {}
    if buffer is not None:
        in_specs.append(pl.BlockSpec(memory_space=pl.ANY))
        operands.append(buffer)
        aliases = {len(operands): 0}
    flops = 2 * count * rows * width * columns
    return pl.pallas_call(
        body,
        out_shape=jax.ShapeDtypeStruct((slot_count, rows, columns), jnp.bfloat16),
        grid_spec=pltpu.PrefetchScalarGridSpec(
            num_scalar_prefetch=1,
            grid=(columns // chunk, count),
            in_specs=in_specs,
            out_specs=pl.BlockSpec((1, rows, chunk), lambda j, i, s: (s[i], 0, j)),
        ),
        input_output_aliases=aliases,
        cost_estimate=pl.CostEstimate(
            flops=flops, bytes_accessed=2 * width * columns, transcendentals=0
        ),
        name="project",
    )(slots, *operands)


def attend(info, head_window, queries, buffer):
    rows, width = queries.shape
    head_size = width // HEADS
    pair_count = width // LANES
    reach = WINDOW // rows
    steps = 2 * reach + 1
    value_first = width // LANES
    cols = 2 * rows

    def body(info_ref, window_ref, query_ref, *refs):
        key_refs = refs[:steps]
        value_refs = refs[steps : 2 * steps]
        out_ref = refs[2 * steps]
        score_ref = refs[2 * steps + 1]
        pair = pl.program_id(0)
        query_first = info_ref[1]
        valid_first = info_ref[2]
        patches = info_ref[3]
        query = query_ref[...]
        lane = lax.broadcasted_iota(jnp.int32, query.shape, 1)
        zero = jnp.zeros_like(query)
        both = jnp.concatenate(
            [jnp.where(lane < head_size, query, zero), jnp.where(lane < head_size, zero, query)], 0
        )
        column = lax.broadcasted_iota(jnp.int32, (1, cols), 1)
        second = column >= rows
        window = jnp.where(second, window_ref[2 * pair + 1], window_ref[2 * pair])
        local = jnp.where(second, column - rows, column)
        lowest = jnp.maximum(local - window, valid_first - query_first)
        highest = jnp.minimum(local + window, patches - 1 - query_first)
        key_row = lax.broadcasted_iota(jnp.int32, (rows, cols), 0)
        largest = None
        for step in range(steps):
            first = (step - reach) * rows
            scores = lax.dot_general(
                key_refs[step][0],
                both,
                (((1,), (1,)), ((), ())),
                preferred_element_type=jnp.float32,
            )
            allowed = None
            if step <= reach:
                allowed = key_row >= lowest - first
            if step >= reach:
                upper = key_row <= highest - first
                allowed = upper if allowed is None else allowed & upper
            scores = jnp.where(allowed, scores, MASKED)
            score_ref[step] = scores
            top = jnp.max(scores, axis=0, keepdims=True)
            largest = top if largest is None else jnp.maximum(largest, top)
        ones = jnp.ones((16, rows), jnp.bfloat16)
        sums = [None, None]
        for step in range(steps):
            weights = jnp.exp2(score_ref[step] - largest).astype(jnp.bfloat16)
            values = value_refs[step][0].T
            for half in range(2):
                left = jnp.concatenate(
                    [values[half * head_size : (half + 1) * head_size], ones], 0
                )
                part = jnp.dot(
                    left,
                    weights[:, half * rows : (half + 1) * rows],
                    preferred_element_type=jnp.float32,
                )
                sums[half] = part if sums[half] is None else sums[half] + part
        query_valid = (
            lax.broadcasted_iota(jnp.int32, (1, rows), 1) >= valid_first - query_first
        )
        outs = []
        for half in range(2):
            factor = jnp.where(query_valid, 1.0 / sums[half][head_size : head_size + 1], 0.0)
            outs.append(sums[half][:head_size] * factor)
        out_ref[...] = jnp.concatenate(outs, 0).T.astype(out_ref.dtype)

    def key_spec(step, offset):
        return pl.BlockSpec(
            (1, rows, LANES), lambda g, info, win: (info[0] - reach + step, 0, offset + g)
        )

    in_specs = [pl.BlockSpec((rows, LANES), lambda g, info, win: (0, g))]
    in_specs += [key_spec(step, 0) for step in range(steps)]
    in_specs += [key_spec(step, value_first) for step in range(steps)]
    return pl.pallas_call(
        body,
        out_shape=jax.ShapeDtypeStruct((rows, width), jnp.bfloat16),
        grid_spec=pltpu.PrefetchScalarGridSpec(
            num_scalar_prefetch=2,
            grid=(pair_count,),
            in_specs=in_specs,
            out_specs=pl.BlockSpec((rows, LANES), lambda g, info, win: (0, g)),
            scratch_shapes=[pltpu.VMEM((steps, rows, cols), jnp.float32)],
        ),
        cost_estimate=pl.CostEstimate(
            flops=8 * steps * rows * rows * width,
            bytes_accessed=4 * steps * rows * width,
            transcendentals=steps * rows * rows * HEADS,
        ),
        name="attend",
    )(info, head_window, queries, *([buffer] * (2 * steps)))


def on_device(
    history, lengths, head_window, input_proj, output_proj, mixer_down, mixer_up, series_mix
):
    local_series, rows, width = history.shape
    devices = lax.axis_size("tm")
    groups = lax.axis_size("series")
    assert local_series == 2 and devices % 4 == 0 and WINDOW == 2 * rows
    patches = rows * devices
    position = lax.axis_index("tm")
    quad, chip, core = position // 4, (position // 2) % 2, position % 2
    chip_swap, core_swap, near_route, far_route = routes(devices)

    def move(block, route):
        return lax.ppermute(block, "tm", route)

    def part(array, index):
        return lax.dynamic_index_in_dim(array, index, 0, keepdims=False)

    mine = part(history, chip)
    other = part(history, 1 - chip)
    away = move(other, chip_swap)
    near = move(mine, near_route)
    mine_beside = move(mine, core_swap)
    far = move(away, far_route)
    away_beside = move(away, core_swap)
    near_beside = move(near, core_swap)
    far_beside = move(far, core_swap)

    home_slot = 2 + 2 * chip
    away_slot = 4 - 2 * chip
    near_slot = 6 - 6 * chip
    far_slot = 6 * chip

    def slots(*firsts):
        return jnp.stack([f + c for f in firsts for c in (core, 1 - core)]).astype(jnp.int32)

    scale = (width // HEADS) ** (-0.5) * math.log2(math.e)

    def query_rows(block):
        return (
            jnp.dot(block, input_proj[:, :width], preferred_element_type=jnp.float32) * scale
        ).astype(jnp.bfloat16)

    valid_first = patches - part(lengths, chip)

    def attention(slot, queries, buffer):
        query_first = (4 * quad - 2 + slot) * rows
        info = jnp.stack([slot, query_first, valid_first, patches]).astype(jnp.int32)
        return attend(info, head_window, queries, buffer)

    buffer = project([mine, mine_beside], slots(home_slot), input_proj, width, 8)
    buffer = project(
        [away, away_beside, near, near_beside],
        slots(away_slot, near_slot),
        input_proj,
        width,
        8,
        buffer,
    )
    away_out = attention(away_slot + core, query_rows(away), buffer)
    other_attended = move(away_out, chip_swap)
    buffer = project([far, far_beside], slots(far_slot), input_proj, width, 8, buffer)
    mine_attended = attention(home_slot + core, query_rows(mine), buffer)

    def finish(rows_in, attended):
        hidden = (
            rows_in.astype(jnp.float32)
            + jnp.dot(attended, output_proj, preferred_element_type=jnp.float32)
        ).astype(jnp.bfloat16)
        branch = jnp.dot(hidden, mixer_down, preferred_element_type=jnp.float32).astype(
            jnp.bfloat16
        )
        return hidden, branch

    own_group = lax.axis_index("series")

    def from_groups(branch):
        gathered = [branch]
        for shift in range(1, groups):
            route = [((g + shift) % groups, g) for g in range(groups)]
            gathered.append(lax.ppermute(branch, "series", route))
        return gathered

    mine_hidden, mine_branch = finish(mine, mine_attended)
    mine_branches = from_groups(mine_branch)
    other_hidden, other_branch = finish(other, other_attended)
    other_branches = from_groups(other_branch)

    mix = series_mix.astype(jnp.float32)

    def combined(which):
        row = part(mix, own_group * 2 + which)
        total = 0.0
        for shift in range(groups):
            group = (own_group + shift) % groups
            total += part(row, group * 2 + chip) * mine_branches[shift].astype(jnp.float32)
            total += part(row, group * 2 + 1 - chip) * other_branches[shift].astype(jnp.float32)
        return total.astype(jnp.bfloat16)

    def output(hidden, which):
        update = jnp.dot(combined(which), mixer_up, preferred_element_type=jnp.float32)
        return (hidden.astype(jnp.float32) + update).astype(jnp.bfloat16)

    mine_out = output(mine_hidden, chip)
    other_out = output(other_hidden, 1 - chip)
    return jnp.where(
        chip == 0, jnp.stack([mine_out, other_out]), jnp.stack([other_out, mine_out])
    )


def solution(mesh):
    in_specs = (P("series", "tm", None), P("series"), P(), P(), P(), P(), P(), P())
    out_specs = P("series", "tm", None)
    return jax.shard_map(
        on_device, mesh=mesh, in_specs=in_specs, out_specs=out_specs, check_vma=False
    )
```

```python
import functools
import math

import jax
import jax.numpy as jnp
from jax import lax
from jax.experimental import pallas as pl
from jax.experimental.pallas import tpu as pltpu
from jax.sharding import PartitionSpec as P

HEADS = 16
WINDOW = 512
LANES = 128
MASKED = -1e30


def routes(count):
    place = lambda quad, chip, core: 4 * quad + 2 * chip + core
    last = count // 4 - 1
    chip_swap = [(i, i ^ 2) for i in range(count)]
    core_swap = [(i, i ^ 1) for i in range(count)]
    near, far = [], []
    for i in range(count):
        quad, chip, core = i // 4, (i // 2) % 2, i % 2
        down = quad - 1 if quad > 0 else None
        up = quad + 1 if quad < last else None
        near_quad, far_quad = (down, up) if chip == 0 else (up, down)
        if near_quad is not None:
            near.append((i, place(near_quad, chip, core)))
        if far_quad is not None:
            far.append((i, place(far_quad, chip, core)))
    return chip_swap, core_swap, near, far


def project(first, beside, weight, scale):
    rows, width = first.shape
    chunk = min(256, width)
    steps = width // chunk

    def body(first_ref, beside_ref, wq_ref, wk_ref, wv_ref, q_ref, k_ref, v_ref):
        def dot(block, ref):
            return jnp.dot(block[...], ref[...], preferred_element_type=jnp.float32)

        q_ref[...] = (dot(first_ref, wq_ref) * scale).astype(jnp.bfloat16)
        for index, block in enumerate((first_ref, beside_ref)):
            k_ref[index] = dot(block, wk_ref).astype(jnp.bfloat16)
            v_ref[index] = dot(block, wv_ref).astype(jnp.bfloat16).T

    whole = pl.BlockSpec((rows, width), lambda g: (0, 0))
    weights = [
        pl.BlockSpec((width, chunk), lambda g, part=part: (0, part * steps + g))
        for part in range(3)
    ]
    return pl.pallas_call(
        body,
        out_shape=(
            jax.ShapeDtypeStruct((rows, width), jnp.bfloat16),
            jax.ShapeDtypeStruct((2, rows, width), jnp.bfloat16),
            jax.ShapeDtypeStruct((2, width, rows), jnp.bfloat16),
        ),
        grid=(steps,),
        in_specs=[whole, whole] + weights,
        out_specs=(
            pl.BlockSpec((rows, chunk), lambda g: (0, g)),
            pl.BlockSpec((2, rows, chunk), lambda g: (0, 0, g)),
            pl.BlockSpec((2, chunk, rows), lambda g: (0, g, 0)),
        ),
        cost_estimate=pl.CostEstimate(
            flops=10 * rows * width * width, bytes_accessed=6 * width * width, transcendentals=0
        ),
        name="project",
    )(first, beside, weight, weight, weight)


def attend(place, head_window, lengths, weight, scale, home, raw, ready, queries=None, keep=0):
    raw_sides = [side for side, _ in raw]
    ready_sides = [side for side, _ in ready]
    raw = [block for _, blocks in raw for block in blocks]
    ready = [arrays for _, arrays in ready]
    rows, width = raw[0].shape
    devices = lax.axis_size("tm")
    head_size = width // HEADS
    pairs = width // LANES
    reach = WINDOW // rows
    steps = 2 * reach + 1
    slot_count = steps + 1
    half_rows = rows // 2
    cols = 2 * half_rows
    raw_count, ready_count = len(raw), len(ready)

    def span(step, half):
        if step == 0 and half == 1:
            return half_rows, rows
        if step == steps - 1 and half == 0:
            return 0, half_rows
        return 0, rows

    def body(place_ref, window_ref, length_ref, *refs):
        refs = list(refs)
        take = lambda count: [refs.pop(0) for _ in range(count)]
        raw_refs = take(raw_count)
        ready_refs = take(2 * ready_count)
        query_ref = take(1)[0] if queries is not None else None
        wq_ref = take(1)[0] if queries is None else None
        wk_ref, wv_ref, out_ref = take(3)
        keep_refs = take(2) if keep else None
        key_scr, weight_scr, row_scr, query_scr = take(4)
        value_scrs, score_scrs, top_scrs = take(2), take(2), take(2)
        index = pl.program_id(0)
        position = place_ref[0]
        core = position % 2
        chip = (position // 2) % 2
        patches = rows * devices
        valid_first = patches - length_ref[chip]
        query_chip = chip if home else 1 - chip
        query_first = (position - 2 * chip + 2 * query_chip) * rows

        def slot_of(side, beside):
            offset = core if not beside else 1 - core
            return 2 + 2 * side * (1 - 2 * chip) + offset

        @pl.when(index == 0)
        def _():
            row_scr[...] = lax.broadcasted_iota(jnp.int32, (rows, LANES), 0)

        def front(parity, value_scr, score_scr, top_scr):
            units = []
            state = {}

            def ready_blocks():
                for number in range(ready_count):
                    for which in range(2):
                        slot = slot_of(ready_sides[number], which)
                        key_scr[slot] = ready_refs[2 * number][which]
                        value_scr[slot] = ready_refs[2 * number + 1][which]
                weight_scr[:, :LANES] = wk_ref[...]
                weight_scr[:, LANES:] = wv_ref[...]

            units.append(ready_blocks)

            def project_queries():
                both = jnp.dot(raw_refs[0][...], wq_ref[...], preferred_element_type=jnp.float32)
                query_scr[...] = (both * scale).astype(jnp.bfloat16)

            if query_ref is None and parity == 0:
                units.append(project_queries)

            def project_block(number, part):
                slot = slot_of(raw_sides[number // 2], number % 2)
                where = slice(part * half_rows, (part + 1) * half_rows)
                both = jnp.dot(
                    raw_refs[number][where, :], weight_scr[...], preferred_element_type=jnp.float32
                ).astype(jnp.bfloat16)
                keys, values = both[:, :LANES], both[:, LANES:].T
                key_scr[slot, where, :] = keys
                value_scr[slot, :, where] = values
                if number < keep:
                    keep_refs[0][number, where, :] = keys
                    keep_refs[1][number, :, where] = values

            for number in range(raw_count):
                for part in range(2):
                    units.append(functools.partial(project_block, number, part))
            early = len(units)

            def bounds(half):
                column = lax.broadcasted_iota(jnp.int32, (1, cols), 1)
                second = column >= half_rows
                window = jnp.where(second, window_ref[2 * index + 1], window_ref[2 * index])
                lane = lax.broadcasted_iota(jnp.int32, (half_rows, LANES), 1)
                local = jnp.where(second, column - half_rows, column) + half * half_rows
                lowest = jnp.maximum(local - window, valid_first - query_first)
                highest = jnp.minimum(local + window, patches - 1 - query_first)
                where = slice(half * half_rows, (half + 1) * half_rows)
                if query_ref is None:
                    part = query_scr[where, parity * LANES : (parity + 1) * LANES]
                else:
                    part = query_ref[where, :]
                zero = jnp.zeros_like(part)
                right = jnp.concatenate(
                    [
                        jnp.where(lane < head_size, part, zero),
                        jnp.where(lane < head_size, zero, part),
                    ],
                    0,
                )
                return right, lowest, highest

            def score_block(half, step):
                if step == 0:
                    state[half] = bounds(half)
                right, lowest, highest = state[half]
                start, stop = span(step, half)
                first = (step - reach) * rows
                scores = lax.dot_general(
                    key_scr[core + step, start:stop, :],
                    right,
                    (((1,), (1,)), ((), ())),
                    preferred_element_type=jnp.float32,
                )
                key_row = row_scr[start:stop, :]
                key_row = jnp.concatenate([key_row] * (cols // LANES), 1)
                allowed = None
                if step <= reach:
                    allowed = key_row >= lowest - first
                if step >= reach:
                    upper = key_row <= highest - first
                    allowed = upper if allowed is None else allowed & upper
                scores = jnp.where(allowed, scores, MASKED)
                score_scr[half, step, start:stop, :] = scores
                top = jnp.max(scores, axis=0, keepdims=True)
                if step > 0:
                    top = jnp.maximum(state["top"], top)
                state["top"] = top
                if step == steps - 1:
                    top_scr[half] = top

            for half in range(2):
                for step in range(steps):
                    units.append(functools.partial(score_block, half, step))
            return units[:early], units[early:]

        def back(value_scr, score_scr, top_scr):
            sums = [None, None]

            def add_block(step, head):
                where = slice(head * half_rows, (head + 1) * half_rows)
                parts = []
                for half in range(2):
                    start, stop = span(step, half)
                    part = jnp.exp2(
                        score_scr[half, step, start:stop, where] - top_scr[half][:, where]
                    )
                    part = [part.astype(jnp.bfloat16)]
                    if start > 0:
                        part = [jnp.zeros((start, half_rows), jnp.bfloat16)] + part
                    if stop < rows:
                        part = part + [jnp.zeros((rows - stop, half_rows), jnp.bfloat16)]
                    parts.append(jnp.concatenate(part, 0) if len(part) > 1 else part[0])
                weights = jnp.concatenate(parts, 1)
                left = jnp.concatenate(
                    [
                        value_scr[core + step, head * head_size : (head + 1) * head_size, :],
                        jnp.ones((16, rows), jnp.bfloat16),
                    ],
                    0,
                )
                add = jnp.dot(left, weights, preferred_element_type=jnp.float32)
                sums[head] = add if sums[head] is None else sums[head] + add

            def write():
                query_valid = (
                    lax.broadcasted_iota(jnp.int32, (1, rows), 1) >= valid_first - query_first
                )
                outs = []
                for head in range(2):
                    total = sums[head][head_size : head_size + 1]
                    factor = jnp.where(query_valid, 1.0 / total, 0.0)
                    outs.append(sums[head][:head_size] * factor)
                out_ref[...] = jnp.concatenate(outs, 0).T.astype(out_ref.dtype)

            units = [
                functools.partial(add_block, step, head)
                for head in range(2)
                for step in range(steps)
            ]
            return units + [write]

        def interleave(first, second):
            done = 0
            for number, unit in enumerate(first):
                unit()
                target = (number + 1) * len(second) // len(first)
                for other in second[done:target]:
                    other()
                done = target

        sets = [(value_scrs[n], score_scrs[n], top_scrs[n]) for n in range(2)]
        for parity in range(2):

            @pl.when((index < pairs) & (index % 2 == parity))
            def _():
                early, late = front(parity, *sets[parity])
                interleave(early, back(*sets[1 - parity]))
                interleave(late, [])

        @pl.when(index == pairs)
        def _():
            for unit in back(*sets[(pairs - 1) % 2]):
                unit()

    ahead = lambda g: jnp.minimum(g, pairs - 1)
    block = pl.BlockSpec((rows, LANES), lambda g, *_: (0, ahead(g)))
    key_spec = lambda count: pl.BlockSpec((count, rows, LANES), lambda g, *_: (0, 0, ahead(g)))
    value_spec = lambda count: pl.BlockSpec((count, LANES, rows), lambda g, *_: (0, ahead(g), 0))
    weight_spec = lambda part: pl.BlockSpec(
        (width, LANES), lambda g, *_: (0, part * pairs + ahead(g))
    )
    in_specs = [pl.BlockSpec((rows, width), lambda g, *_: (0, 0)) for _ in raw]
    operands = list(raw)
    for keys, values in ready:
        in_specs += [key_spec(2), value_spec(2)]
        operands += [keys, values]
    if queries is not None:
        in_specs.append(block)
        operands.append(queries)
    else:
        in_specs.append(
            pl.BlockSpec((width, 2 * LANES), lambda g, *_: (0, ahead(g) // 2))
        )
        operands.append(weight)
    in_specs += [weight_spec(1), weight_spec(2)]
    operands += [weight, weight]
    out_shape = [jax.ShapeDtypeStruct((rows, width), jnp.bfloat16)]
    out_specs = [pl.BlockSpec((rows, LANES), lambda g, *_: (0, jnp.maximum(g - 1, 0)))]
    if keep:
        out_shape += [
            jax.ShapeDtypeStruct((keep, rows, width), jnp.bfloat16),
            jax.ShapeDtypeStruct((keep, width, rows), jnp.bfloat16),
        ]
        out_specs += [key_spec(keep), value_spec(keep)]
    twice = lambda shape, dtype: [pltpu.VMEM(shape, dtype)] * 2
    return pl.pallas_call(
        body,
        out_shape=tuple(out_shape),
        grid_spec=pltpu.PrefetchScalarGridSpec(
            num_scalar_prefetch=3,
            grid=(pairs + 1,),
            in_specs=in_specs,
            out_specs=tuple(out_specs),
            scratch_shapes=[
                pltpu.VMEM((slot_count, rows, LANES), jnp.bfloat16),
                pltpu.VMEM((width, 2 * LANES), jnp.bfloat16),
                pltpu.VMEM((rows, LANES), jnp.int32),
                pltpu.VMEM((rows, 2 * LANES), jnp.bfloat16),
            ]
            + twice((slot_count, LANES, rows), jnp.bfloat16)
            + twice((2, steps, rows, cols), jnp.float32)
            + twice((2, 1, cols), jnp.float32),
        ),
        cost_estimate=pl.CostEstimate(
            flops=(8 * steps * rows + 4 * raw_count * width) * rows * width,
            bytes_accessed=4 * width * width + 4 * steps * rows * width,
            transcendentals=steps * rows * rows * HEADS,
        ),
        name="attend",
    )(place, head_window, lengths, *operands)


def mix(place, own_group, series_mix, weight, hidden, branches):
    rows, width = hidden[0].shape
    inner = weight.shape[0]
    groups = len(branches[0])

    def body(place_ref, group_ref, mix_ref, weight_ref, *refs):
        hidden_refs = refs[:2]
        branch_refs = refs[2 : 2 + 2 * groups]
        out_ref = refs[-1]
        own = group_ref[0]
        chip = (place_ref[0] // 2) % 2
        for which in range(2):

            @pl.when(pl.program_id(0) == which)
            def _():
                series = [chip, 1 - chip]
                row = 2 * own + series[which]
                total = None
                for number, branch_ref in enumerate(branch_refs):
                    kind, shift = number // groups, number % groups
                    group = (own + shift) % groups
                    term = mix_ref[row, 2 * group + series[kind]] * branch_ref[...].astype(
                        jnp.float32
                    )
                    total = term if total is None else total + term
                update = jnp.dot(
                    total.astype(jnp.bfloat16), weight_ref[...], preferred_element_type=jnp.float32
                )
                out_ref[0] = (hidden_refs[which][...].astype(jnp.float32) + update).astype(
                    out_ref.dtype
                )

    def out_index(which, place_ref, *_):
        chip = (place_ref[0] // 2) % 2
        return chip + which - 2 * chip * which, 0, 0

    whole = lambda shape: pl.BlockSpec(shape, lambda which, *_: (0, 0))
    return pl.pallas_call(
        body,
        out_shape=jax.ShapeDtypeStruct((2, rows, width), jnp.bfloat16),
        grid_spec=pltpu.PrefetchScalarGridSpec(
            num_scalar_prefetch=3,
            grid=(2,),
            in_specs=[whole((inner, width))]
            + [whole((rows, width))] * 2
            + [whole((rows, inner))] * (2 * groups),
            out_specs=pl.BlockSpec((1, rows, width), out_index),
        ),
        cost_estimate=pl.CostEstimate(
            flops=4 * rows * inner * width, bytes_accessed=2 * inner * width, transcendentals=0
        ),
        name="mix",
    )(place, own_group, series_mix, weight, *hidden, *branches[0], *branches[1])


def on_device(
    history, lengths, head_window, input_proj, output_proj, mixer_down, mixer_up, series_mix
):
    local_series, rows, width = history.shape
    devices = lax.axis_size("tm")
    groups = lax.axis_size("series")
    assert local_series == 2 and devices % 4 == 0 and WINDOW == 2 * rows
    patches = rows * devices
    position = lax.axis_index("tm")
    quad, chip, core = position // 4, (position // 2) % 2, position % 2
    chip_swap, core_swap, near_route, far_route = routes(devices)

    def move(block, route):
        return lax.ppermute(block, "tm", route)

    def part(array, index):
        return lax.dynamic_index_in_dim(array, index, 0, keepdims=False)

    mine = part(history, chip)
    other = part(history, 1 - chip)
    away = move(other, chip_swap)
    near = move(mine, near_route)
    mine_beside = move(mine, core_swap)
    scale = (width // HEADS) ** (-0.5) * math.log2(math.e)
    place = position.astype(jnp.int32)[None]
    attention = functools.partial(attend, place, head_window, lengths, input_proj, scale)

    home_queries, *home_ready = project(mine, mine_beside, input_proj, scale)
    away, home_queries = lax.optimization_barrier((away, home_queries))
    far = move(away, far_route)
    away_beside = move(away, core_swap)
    near, home_queries = lax.optimization_barrier((near, home_queries))
    near_beside = move(near, core_swap)
    away_out, *away_ready = attention(
        False,
        [(0, [away, away_beside]), (1, [near, near_beside])],
        [(-1, home_ready)],
        keep=2,
    )
    away_out, far = lax.optimization_barrier((away_out, far))
    other_attended = move(away_out, chip_swap)
    far_beside = move(far, core_swap)
    (mine_attended,) = attention(
        True,
        [(-1, [far, far_beside])],
        [(0, home_ready), (1, away_ready)],
        queries=home_queries,
    )

    def finish(rows_in, attended):
        hidden = (
            rows_in.astype(jnp.float32)
            + jnp.dot(attended, output_proj, preferred_element_type=jnp.float32)
        ).astype(jnp.bfloat16)
        branch = jnp.dot(hidden, mixer_down, preferred_element_type=jnp.float32).astype(
            jnp.bfloat16
        )
        return hidden, branch

    own_group = lax.axis_index("series")

    def from_groups(branch):
        gathered = [branch]
        for shift in range(1, groups):
            route = [((g + shift) % groups, g) for g in range(groups)]
            gathered.append(lax.ppermute(branch, "series", route))
        return gathered

    mine_hidden, mine_branch = finish(mine, mine_attended)
    mine_branches = from_groups(mine_branch)
    other_attended, mine_attended = lax.optimization_barrier((other_attended, mine_attended))
    other_hidden, other_branch = finish(other, other_attended)
    other_branches = from_groups(other_branch)

    return mix(
        place,
        own_group.astype(jnp.int32)[None],
        series_mix.astype(jnp.float32),
        mixer_up,
        (mine_hidden, other_hidden),
        (mine_branches, other_branches),
    )


def solution(mesh):
    in_specs = (P("series", "tm", None), P("series"), P(), P(), P(), P(), P(), P())
    out_specs = P("series", "tm", None)
    return jax.shard_map(
        on_device, mesh=mesh, in_specs=in_specs, out_specs=out_specs, check_vma=False
    )
```

```python
import functools
import math

import jax
import jax.numpy as jnp
from jax import lax
from jax.experimental import pallas as pl
from jax.experimental.pallas import tpu as pltpu
from jax.sharding import PartitionSpec as P

HEADS = 16
WINDOW = 512
LANES = 128
MASKED = -1e30


def routes(count):
    place = lambda quad, chip, core: 4 * quad + 2 * chip + core
    last = count // 4 - 1
    chip_swap = [(i, i ^ 2) for i in range(count)]
    core_swap = [(i, i ^ 1) for i in range(count)]
    near, far = [], []
    for i in range(count):
        quad, chip, core = i // 4, (i // 2) % 2, i % 2
        down = quad - 1 if quad > 0 else None
        up = quad + 1 if quad < last else None
        near_quad, far_quad = (down, up) if chip == 0 else (up, down)
        if near_quad is not None:
            near.append((i, place(near_quad, chip, core)))
        if far_quad is not None:
            far.append((i, place(far_quad, chip, core)))
    return chip_swap, core_swap, near, far


def project(first, beside, weight, scale):
    rows, width = first.shape
    chunk = min(256, width)
    steps = width // chunk

    def body(first_ref, beside_ref, wq_ref, wk_ref, wv_ref, q_ref, k_ref, v_ref):
        def dot(block, ref):
            return jnp.dot(block[...], ref[...], preferred_element_type=jnp.float32)

        q_ref[...] = (dot(first_ref, wq_ref) * scale).astype(jnp.bfloat16)
        for index, block in enumerate((first_ref, beside_ref)):
            k_ref[index] = dot(block, wk_ref).astype(jnp.bfloat16)
            v_ref[index] = dot(block, wv_ref).astype(jnp.bfloat16).T

    whole = pl.BlockSpec((rows, width), lambda g: (0, 0))
    weights = [
        pl.BlockSpec((width, chunk), lambda g, part=part: (0, part * steps + g))
        for part in range(3)
    ]
    return pl.pallas_call(
        body,
        out_shape=(
            jax.ShapeDtypeStruct((rows, width), jnp.bfloat16),
            jax.ShapeDtypeStruct((2, rows, width), jnp.bfloat16),
            jax.ShapeDtypeStruct((2, width, rows), jnp.bfloat16),
        ),
        grid=(steps,),
        in_specs=[whole, whole] + weights,
        out_specs=(
            pl.BlockSpec((rows, chunk), lambda g: (0, g)),
            pl.BlockSpec((2, rows, chunk), lambda g: (0, 0, g)),
            pl.BlockSpec((2, chunk, rows), lambda g: (0, g, 0)),
        ),
        cost_estimate=pl.CostEstimate(
            flops=10 * rows * width * width, bytes_accessed=6 * width * width, transcendentals=0
        ),
        name="project",
    )(first, beside, weight, weight, weight)


def attend(
    place, head_window, lengths, weight, output_proj, mixer_down, scale, home, raw, ready,
    own=None, keep=0,
):
    raw_sides = [side for side, _ in raw]
    ready_sides = [side for side, _ in ready]
    raw = [block for _, blocks in raw for block in blocks]
    ready = [arrays for _, arrays in ready]
    rows, width = raw[0].shape
    devices = lax.axis_size("tm")
    head_size = width // HEADS
    pairs = width // LANES
    reach = WINDOW // rows
    steps = 2 * reach + 1
    slot_count = steps + 1
    half_rows = rows // 2
    cols = 2 * half_rows
    raw_count, ready_count = len(raw), len(ready)

    def span(step, half):
        if step == 0 and half == 1:
            return half_rows, rows
        if step == steps - 1 and half == 0:
            return 0, half_rows
        return 0, rows

    def body(place_ref, window_ref, length_ref, *refs):
        refs = list(refs)
        take = lambda count: [refs.pop(0) for _ in range(count)]
        raw_refs = take(raw_count)
        ready_refs = take(2 * ready_count)
        rows_ref, query_ref = take(2) if home else (raw_refs[0], None)
        wq_ref = None if home else take(1)[0]
        wk_ref, wv_ref, wo_hbm, down_hbm = take(4)
        hidden_ref, branch_ref = take(2)
        keep_refs = take(2) if keep else None
        key_scr, weight_scr, row_scr, query_scr = take(4)
        value_scrs, score_scrs, top_scrs = take(2), take(2), take(2)
        attended_scr, wo_scr, down_scr, copy_sems = take(4)
        index = pl.program_id(0)
        position = place_ref[0]
        core = position % 2
        chip = (position // 2) % 2
        patches = rows * devices
        valid_first = patches - length_ref[chip]
        query_chip = chip if home else 1 - chip
        query_first = (position - 2 * chip + 2 * query_chip) * rows

        def slot_of(side, beside):
            offset = core if not beside else 1 - core
            return 2 + 2 * side * (1 - 2 * chip) + offset

        copies = [
            pltpu.make_async_copy(wo_hbm, wo_scr, copy_sems.at[0]),
            pltpu.make_async_copy(down_hbm, down_scr, copy_sems.at[1]),
        ]

        @pl.when(index == 0)
        def _():
            for copy in copies:
                copy.start()
            row_scr[...] = lax.broadcasted_iota(jnp.int32, (rows, LANES), 0)

        def front(parity, value_scr, score_scr, top_scr):
            units = []
            state = {}

            def ready_blocks():
                for number in range(ready_count):
                    for which in range(2):
                        slot = slot_of(ready_sides[number], which)
                        key_scr[slot] = ready_refs[2 * number][which]
                        value_scr[slot] = ready_refs[2 * number + 1][which]
                weight_scr[:, :LANES] = wk_ref[...]
                weight_scr[:, LANES:] = wv_ref[...]

            units.append(ready_blocks)

            def project_queries():
                both = jnp.dot(raw_refs[0][...], wq_ref[...], preferred_element_type=jnp.float32)
                query_scr[...] = (both * scale).astype(jnp.bfloat16)

            if query_ref is None and parity == 0:
                units.append(project_queries)

            def project_block(number, part):
                slot = slot_of(raw_sides[number // 2], number % 2)
                where = slice(part * half_rows, (part + 1) * half_rows)
                both = jnp.dot(
                    raw_refs[number][where, :], weight_scr[...], preferred_element_type=jnp.float32
                ).astype(jnp.bfloat16)
                keys, values = both[:, :LANES], both[:, LANES:].T
                key_scr[slot, where, :] = keys
                value_scr[slot, :, where] = values
                if number < keep:
                    keep_refs[0][number, where, :] = keys
                    keep_refs[1][number, :, where] = values

            for number in range(raw_count):
                for part in range(2):
                    units.append(functools.partial(project_block, number, part))
            early = len(units)

            def bounds(half):
                column = lax.broadcasted_iota(jnp.int32, (1, cols), 1)
                second = column >= half_rows
                window = jnp.where(second, window_ref[2 * index + 1], window_ref[2 * index])
                lane = lax.broadcasted_iota(jnp.int32, (half_rows, LANES), 1)
                local = jnp.where(second, column - half_rows, column) + half * half_rows
                lowest = jnp.maximum(local - window, valid_first - query_first)
                highest = jnp.minimum(local + window, patches - 1 - query_first)
                where = slice(half * half_rows, (half + 1) * half_rows)
                if query_ref is None:
                    part = query_scr[where, parity * LANES : (parity + 1) * LANES]
                else:
                    part = query_ref[where, :]
                zero = jnp.zeros_like(part)
                right = jnp.concatenate(
                    [
                        jnp.where(lane < head_size, part, zero),
                        jnp.where(lane < head_size, zero, part),
                    ],
                    0,
                )
                return right, lowest, highest

            def score_block(half, step):
                if step == 0:
                    state[half] = bounds(half)
                right, lowest, highest = state[half]
                start, stop = span(step, half)
                first = (step - reach) * rows
                scores = lax.dot_general(
                    key_scr[core + step, start:stop, :],
                    right,
                    (((1,), (1,)), ((), ())),
                    preferred_element_type=jnp.float32,
                )
                key_row = row_scr[start:stop, :]
                key_row = jnp.concatenate([key_row] * (cols // LANES), 1)
                allowed = None
                if step <= reach:
                    allowed = key_row >= lowest - first
                if step >= reach:
                    upper = key_row <= highest - first
                    allowed = upper if allowed is None else allowed & upper
                scores = jnp.where(allowed, scores, MASKED)
                score_scr[half, step, start:stop, :] = scores
                top = jnp.max(scores, axis=0, keepdims=True)
                if step > 0:
                    top = jnp.maximum(state["top"], top)
                state["top"] = top
                if step == steps - 1:
                    top_scr[half] = top

            for half in range(2):
                for step in range(steps):
                    units.append(functools.partial(score_block, half, step))
            return units[:early], units[early:]

        def back(value_scr, score_scr, top_scr):
            sums = [None, None]

            def add_block(step, head):
                where = slice(head * half_rows, (head + 1) * half_rows)
                parts = []
                for half in range(2):
                    start, stop = span(step, half)
                    part = jnp.exp2(
                        score_scr[half, step, start:stop, where] - top_scr[half][:, where]
                    )
                    part = [part.astype(jnp.bfloat16)]
                    if start > 0:
                        part = [jnp.zeros((start, half_rows), jnp.bfloat16)] + part
                    if stop < rows:
                        part = part + [jnp.zeros((rows - stop, half_rows), jnp.bfloat16)]
                    parts.append(jnp.concatenate(part, 0) if len(part) > 1 else part[0])
                weights = jnp.concatenate(parts, 1)
                left = jnp.concatenate(
                    [
                        value_scr[core + step, head * head_size : (head + 1) * head_size, :],
                        jnp.ones((16, rows), jnp.bfloat16),
                    ],
                    0,
                )
                add = jnp.dot(left, weights, preferred_element_type=jnp.float32)
                sums[head] = add if sums[head] is None else sums[head] + add

            def write():
                query_valid = (
                    lax.broadcasted_iota(jnp.int32, (1, rows), 1) >= valid_first - query_first
                )
                outs = []
                for head in range(2):
                    total = sums[head][head_size : head_size + 1]
                    factor = jnp.where(query_valid, 1.0 / total, 0.0)
                    outs.append(sums[head][:head_size] * factor)
                where = pl.ds(pl.multiple_of(jnp.maximum(index - 1, 0) * LANES, LANES), LANES)
                attended_scr[:, where] = jnp.concatenate(outs, 0).T.astype(jnp.bfloat16)

            units = [
                functools.partial(add_block, step, head)
                for head in range(2)
                for step in range(steps)
            ]
            return units + [write]

        def interleave(first, second):
            done = 0
            for number, unit in enumerate(first):
                unit()
                target = (number + 1) * len(second) // len(first)
                for other in second[done:target]:
                    other()
                done = target

        sets = [(value_scrs[n], score_scrs[n], top_scrs[n]) for n in range(2)]
        for parity in range(2):

            @pl.when((index < pairs) & (index % 2 == parity))
            def _():
                early, late = front(parity, *sets[parity])
                interleave(early, back(*sets[1 - parity]))
                interleave(late, [])

        @pl.when(index == pairs)
        def _():
            for unit in back(*sets[(pairs - 1) % 2]):
                unit()
            for copy in copies:
                copy.wait()
            update = jnp.dot(attended_scr[...], wo_scr[...], preferred_element_type=jnp.float32)
            hidden = (rows_ref[...].astype(jnp.float32) + update).astype(jnp.bfloat16)
            hidden_ref[...] = hidden
            branch_ref[...] = jnp.dot(
                hidden, down_scr[...], preferred_element_type=jnp.float32
            ).astype(jnp.bfloat16)

    ahead = lambda g: jnp.minimum(g, pairs - 1)
    block = pl.BlockSpec((rows, LANES), lambda g, *_: (0, ahead(g)))
    key_spec = lambda count: pl.BlockSpec((count, rows, LANES), lambda g, *_: (0, 0, ahead(g)))
    value_spec = lambda count: pl.BlockSpec((count, LANES, rows), lambda g, *_: (0, ahead(g), 0))
    weight_spec = lambda part: pl.BlockSpec(
        (width, LANES), lambda g, *_: (0, part * pairs + ahead(g))
    )
    in_specs = [pl.BlockSpec((rows, width), lambda g, *_: (0, 0)) for _ in raw]
    operands = list(raw)
    for keys, values in ready:
        in_specs += [key_spec(2), value_spec(2)]
        operands += [keys, values]
    whole = lambda shape: pl.BlockSpec(shape, lambda g, *_: (0, 0))
    if home:
        in_specs += [whole((rows, width)), block]
        operands += own
    else:
        in_specs.append(
            pl.BlockSpec((width, 2 * LANES), lambda g, *_: (0, ahead(g) // 2))
        )
        operands.append(weight)
    in_specs += [weight_spec(1), weight_spec(2)] + [pl.BlockSpec(memory_space=pl.ANY)] * 2
    operands += [weight, weight, output_proj, mixer_down]
    inner = mixer_down.shape[1]
    out_shape = [
        jax.ShapeDtypeStruct((rows, width), jnp.bfloat16),
        jax.ShapeDtypeStruct((rows, inner), jnp.bfloat16),
    ]
    out_specs = [whole((rows, width)), whole((rows, inner))]
    if keep:
        out_shape += [
            jax.ShapeDtypeStruct((keep, rows, width), jnp.bfloat16),
            jax.ShapeDtypeStruct((keep, width, rows), jnp.bfloat16),
        ]
        out_specs += [key_spec(keep), value_spec(keep)]
    twice = lambda shape, dtype: [pltpu.VMEM(shape, dtype)] * 2
    return pl.pallas_call(
        body,
        out_shape=tuple(out_shape),
        grid_spec=pltpu.PrefetchScalarGridSpec(
            num_scalar_prefetch=3,
            grid=(pairs + 1,),
            in_specs=in_specs,
            out_specs=tuple(out_specs),
            scratch_shapes=[
                pltpu.VMEM((slot_count, rows, LANES), jnp.bfloat16),
                pltpu.VMEM((width, 2 * LANES), jnp.bfloat16),
                pltpu.VMEM((rows, LANES), jnp.int32),
                pltpu.VMEM((rows, 2 * LANES), jnp.bfloat16),
            ]
            + twice((slot_count, LANES, rows), jnp.bfloat16)
            + twice((2, steps, rows, cols), jnp.float32)
            + twice((2, 1, cols), jnp.float32)
            + [
                pltpu.VMEM((rows, width), jnp.bfloat16),
                pltpu.VMEM(output_proj.shape, jnp.bfloat16),
                pltpu.VMEM(mixer_down.shape, jnp.bfloat16),
                pltpu.SemaphoreType.DMA((2,)),
            ],
        ),
        cost_estimate=pl.CostEstimate(
            flops=(8 * steps * rows + 4 * raw_count * width) * rows * width,
            bytes_accessed=4 * width * width + 4 * steps * rows * width,
            transcendentals=steps * rows * rows * HEADS,
        ),
        name="attend",
    )(place, head_window, lengths, *operands)


def mix(place, own_group, series_mix, weight, hidden, branches):
    rows, width = hidden[0].shape
    inner = weight.shape[0]
    groups = len(branches[0])

    def body(place_ref, group_ref, mix_ref, weight_ref, *refs):
        hidden_refs = refs[:2]
        branch_refs = refs[2 : 2 + 2 * groups]
        out_ref = refs[-1]
        own = group_ref[0]
        chip = (place_ref[0] // 2) % 2
        for which in range(2):

            @pl.when(pl.program_id(0) == which)
            def _():
                series = [chip, 1 - chip]
                row = 2 * own + series[which]
                total = None
                for number, branch_ref in enumerate(branch_refs):
                    kind, shift = number // groups, number % groups
                    group = (own + shift) % groups
                    term = mix_ref[row, 2 * group + series[kind]] * branch_ref[...].astype(
                        jnp.float32
                    )
                    total = term if total is None else total + term
                update = jnp.dot(
                    total.astype(jnp.bfloat16), weight_ref[...], preferred_element_type=jnp.float32
                )
                out_ref[0] = (hidden_refs[which][...].astype(jnp.float32) + update).astype(
                    out_ref.dtype
                )

    def out_index(which, place_ref, *_):
        chip = (place_ref[0] // 2) % 2
        return chip + which - 2 * chip * which, 0, 0

    whole = lambda shape: pl.BlockSpec(shape, lambda which, *_: (0, 0))
    return pl.pallas_call(
        body,
        out_shape=jax.ShapeDtypeStruct((2, rows, width), jnp.bfloat16),
        grid_spec=pltpu.PrefetchScalarGridSpec(
            num_scalar_prefetch=3,
            grid=(2,),
            in_specs=[whole((inner, width))]
            + [whole((rows, width))] * 2
            + [whole((rows, inner))] * (2 * groups),
            out_specs=pl.BlockSpec((1, rows, width), out_index),
        ),
        cost_estimate=pl.CostEstimate(
            flops=4 * rows * inner * width, bytes_accessed=2 * inner * width, transcendentals=0
        ),
        name="mix",
    )(place, own_group, series_mix, weight, *hidden, *branches[0], *branches[1])


def on_device(
    history, lengths, head_window, input_proj, output_proj, mixer_down, mixer_up, series_mix
):
    local_series, rows, width = history.shape
    devices = lax.axis_size("tm")
    groups = lax.axis_size("series")
    assert local_series == 2 and devices % 4 == 0 and WINDOW == 2 * rows
    patches = rows * devices
    position = lax.axis_index("tm")
    quad, chip, core = position // 4, (position // 2) % 2, position % 2
    chip_swap, core_swap, near_route, far_route = routes(devices)

    def move(block, route):
        return lax.ppermute(block, "tm", route)

    def part(array, index):
        return lax.dynamic_index_in_dim(array, index, 0, keepdims=False)

    mine = part(history, chip)
    other = part(history, 1 - chip)
    away = move(other, chip_swap)
    near = move(mine, near_route)
    mine_beside = move(mine, core_swap)
    scale = (width // HEADS) ** (-0.5) * math.log2(math.e)
    place = position.astype(jnp.int32)[None]
    attention = functools.partial(
        attend, place, head_window, lengths, input_proj, output_proj, mixer_down, scale
    )

    home_queries, *home_ready = project(mine, mine_beside, input_proj, scale)
    away, home_queries = lax.optimization_barrier((away, home_queries))
    far = move(away, far_route)
    away_beside = move(away, core_swap)
    near, home_queries = lax.optimization_barrier((near, home_queries))
    near_beside = move(near, core_swap)
    away_hidden, away_branch, *away_ready = attention(
        False,
        [(0, [away, away_beside]), (1, [near, near_beside])],
        [(-1, home_ready)],
        keep=2,
    )
    away_hidden, far = lax.optimization_barrier((away_hidden, far))
    far_beside = move(far, core_swap)

    def down(hidden):
        return jnp.dot(hidden, mixer_down, preferred_element_type=jnp.float32).astype(jnp.bfloat16)

    other_hidden = move(away_hidden, chip_swap)
    other_branches = []
    for shift in range(1, groups):
        route = [
            (i * groups + (g + shift) % groups, home * groups + g)
            for g in range(groups)
            for i, home in chip_swap
        ]
        other_branches.append(lax.ppermute(away_branch, ("tm", "series"), route))

    mine_hidden, mine_branch = attention(
        True,
        [(-1, [far, far_beside])],
        [(0, home_ready), (1, away_ready)],
        own=[mine, home_queries],
    )
    mine_branches = [mine_branch]
    for shift in range(1, groups):
        route = [((g + shift) % groups, g) for g in range(groups)]
        mine_branches.append(lax.ppermute(mine_branch, "series", route))
    other_hidden, mine_branch = lax.optimization_barrier((other_hidden, mine_branch))
    other_branches = [down(other_hidden)] + other_branches

    own_group = lax.axis_index("series")
    return mix(
        place,
        own_group.astype(jnp.int32)[None],
        series_mix.astype(jnp.float32),
        mixer_up,
        (mine_hidden, other_hidden),
        (mine_branches, other_branches),
    )


def solution(mesh):
    in_specs = (P("series", "tm", None), P("series"), P(), P(), P(), P(), P(), P())
    out_specs = P("series", "tm", None)
    return jax.shard_map(
        on_device, mesh=mesh, in_specs=in_specs, out_specs=out_specs, check_vma=False
    )
```

```python
import functools
import math

import jax
import jax.numpy as jnp
from jax import lax
from jax.experimental import pallas as pl
from jax.experimental.pallas import tpu as pltpu
from jax.sharding import PartitionSpec as P

HEADS = 16
WINDOW = 512
LANES = 128
MASKED = -1e30


def routes(count):
    place = lambda quad, chip, core: 4 * quad + 2 * chip + core
    last = count // 4 - 1
    chip_swap = [(i, i ^ 2) for i in range(count)]
    core_swap = [(i, i ^ 1) for i in range(count)]
    near, far, far_cross = [], [], []
    for i in range(count):
        quad, chip, core = i // 4, (i // 2) % 2, i % 2
        down = quad - 1 if quad > 0 else None
        up = quad + 1 if quad < last else None
        near_quad, far_quad = (down, up) if chip == 0 else (up, down)
        if near_quad is not None:
            near.append((i, place(near_quad, chip, core)))
        if far_quad is not None:
            far.append((i, place(far_quad, chip, core)))
            if core != chip:
                far_cross.append((i, place(far_quad, chip, chip)))
    return chip_swap, core_swap, near, far, far_cross


def project(first, beside, weight, scale):
    rows, width = first.shape
    chunk = min(256, width)
    steps = width // chunk

    def body(first_ref, beside_ref, wq_ref, wk_ref, wv_ref, q_ref, k_ref, v_ref):
        def dot(block, ref):
            return jnp.dot(block[...], ref[...], preferred_element_type=jnp.float32)

        q_ref[...] = (dot(first_ref, wq_ref) * scale).astype(jnp.bfloat16)
        for index, block in enumerate((first_ref, beside_ref)):
            k_ref[index] = dot(block, wk_ref).astype(jnp.bfloat16)
            v_ref[index] = dot(block, wv_ref).astype(jnp.bfloat16).T

    whole = pl.BlockSpec((rows, width), lambda g: (0, 0))
    weights = [
        pl.BlockSpec((width, chunk), lambda g, part=part: (0, part * steps + g))
        for part in range(3)
    ]
    return pl.pallas_call(
        body,
        out_shape=(
            jax.ShapeDtypeStruct((rows, width), jnp.bfloat16),
            jax.ShapeDtypeStruct((2, rows, width), jnp.bfloat16),
            jax.ShapeDtypeStruct((2, width, rows), jnp.bfloat16),
        ),
        grid=(steps,),
        in_specs=[whole, whole] + weights,
        out_specs=(
            pl.BlockSpec((rows, chunk), lambda g: (0, g)),
            pl.BlockSpec((2, rows, chunk), lambda g: (0, 0, g)),
            pl.BlockSpec((2, chunk, rows), lambda g: (0, g, 0)),
        ),
        cost_estimate=pl.CostEstimate(
            flops=10 * rows * width * width, bytes_accessed=6 * width * width, transcendentals=0
        ),
        name="project",
    )(first, beside, weight, weight, weight)


def attend(
    place, head_window, lengths, weight, output_proj, mixer_down, scale, home, raw, ready,
    own=None, keep=0,
):
    raw_sides = [side for side, _ in raw]
    ready_sides = [side for side, _ in ready]
    raw = [block for _, blocks in raw for block in blocks]
    ready = [arrays for _, arrays in ready]
    rows, width = raw[0].shape
    devices = lax.axis_size("tm")
    head_size = width // HEADS
    chunk = 2 * LANES
    chunks = width // chunk
    pairs = chunk // LANES
    reach = WINDOW // rows
    steps = 2 * reach + 1
    slot_count = steps + 1
    half_rows = rows // 2
    cols = 2 * half_rows
    raw_count, ready_count = len(raw), len(ready)

    def span(step, half):
        if step == 0 and half == 1:
            return half_rows, rows
        if step == steps - 1 and half == 0:
            return 0, half_rows
        return 0, rows

    def body(place_ref, window_ref, length_ref, *refs):
        refs = list(refs)
        take = lambda count: [refs.pop(0) for _ in range(count)]
        raw_refs = take(raw_count)
        ready_refs = take(2 * ready_count)
        rows_ref, query_ref = take(2) if home else (raw_refs[0], None)
        wq_ref = None if home else take(1)[0]
        wk_ref, wv_ref, wo_hbm, down_hbm = take(4)
        hidden_ref, branch_ref = take(2)
        keep_refs = take(2) if keep else None
        key_scr, row_scr, query_scr = take(3)
        value_scrs, score_scrs, top_scrs = take(2), take(2), take(2)
        attended_scr, wo_scr, down_scr, copy_sems = take(4)
        index = pl.program_id(0)
        position = place_ref[0]
        core = position % 2
        chip = (position // 2) % 2
        patches = rows * devices
        valid_first = patches - length_ref[chip]
        query_chip = chip if home else 1 - chip
        query_first = (position - 2 * chip + 2 * query_chip) * rows

        def slot_of(side, beside):
            offset = core if not beside else 1 - core
            return 2 + 2 * side * (1 - 2 * chip) + offset

        copies = [
            pltpu.make_async_copy(wo_hbm, wo_scr, copy_sems.at[0]),
            pltpu.make_async_copy(down_hbm, down_scr, copy_sems.at[1]),
        ]

        @pl.when(index == 0)
        def _():
            for copy in copies:
                copy.start()
            row_scr[...] = lax.broadcasted_iota(jnp.int32, (rows, LANES), 0)

        def front(value_scr, score_scr, top_scr):
            units = []
            state = {}

            def ready_blocks():
                for number in range(ready_count):
                    for which in range(2):
                        slot = slot_of(ready_sides[number], which)
                        key_scr[slot] = ready_refs[2 * number][which]
                        value_scr[slot] = ready_refs[2 * number + 1][which]

            units.append(ready_blocks)

            def project_queries():
                both = jnp.dot(raw_refs[0][...], wq_ref[...], preferred_element_type=jnp.float32)
                query_scr[...] = (both * scale).astype(jnp.bfloat16)

            if query_ref is None:
                units.append(project_queries)

            def project_keys(number):
                slot = slot_of(raw_sides[number // 2], number % 2)
                keys = jnp.dot(
                    raw_refs[number][...], wk_ref[...], preferred_element_type=jnp.float32
                ).astype(jnp.bfloat16)
                key_scr[slot] = keys
                if number < keep:
                    keep_refs[0][number] = keys

            def project_values(number):
                slot = slot_of(raw_sides[number // 2], number % 2)
                values = jnp.dot(
                    raw_refs[number][...], wv_ref[...], preferred_element_type=jnp.float32
                ).astype(jnp.bfloat16).T
                value_scr[slot] = values
                if number < keep:
                    keep_refs[1][number] = values

            for project in (project_keys, project_values):
                for number in range(raw_count):
                    units.append(functools.partial(project, number))
            early = len(units)

            def bounds(pair, half):
                column = lax.broadcasted_iota(jnp.int32, (1, cols), 1)
                second = column >= half_rows
                head = 2 * (pairs * index + pair)
                window = jnp.where(second, window_ref[head + 1], window_ref[head])
                lane = lax.broadcasted_iota(jnp.int32, (half_rows, LANES), 1)
                local = jnp.where(second, column - half_rows, column) + half * half_rows
                lowest = jnp.maximum(local - window, valid_first - query_first)
                highest = jnp.minimum(local + window, patches - 1 - query_first)
                where = slice(half * half_rows, (half + 1) * half_rows)
                source = query_scr if query_ref is None else query_ref
                part = source[where, pair * LANES : (pair + 1) * LANES]
                zero = jnp.zeros_like(part)
                right = jnp.concatenate(
                    [
                        jnp.where(lane < head_size, part, zero),
                        jnp.where(lane < head_size, zero, part),
                    ],
                    0,
                )
                return right, lowest, highest

            def score_block(pair, half, step):
                if step == 0:
                    state["bounds"] = bounds(pair, half)
                right, lowest, highest = state["bounds"]
                start, stop = span(step, half)
                first = (step - reach) * rows
                scores = lax.dot_general(
                    key_scr[core + step, start:stop, pair * LANES : (pair + 1) * LANES],
                    right,
                    (((1,), (1,)), ((), ())),
                    preferred_element_type=jnp.float32,
                )
                key_row = row_scr[start:stop, :]
                key_row = jnp.concatenate([key_row] * (cols // LANES), 1)
                allowed = None
                if step <= reach:
                    allowed = key_row >= lowest - first
                if step >= reach:
                    upper = key_row <= highest - first
                    allowed = upper if allowed is None else allowed & upper
                scores = jnp.where(allowed, scores, MASKED)
                score_scr[pair, half, step, start:stop, :] = scores
                top = jnp.max(scores, axis=0, keepdims=True)
                if step > 0:
                    top = jnp.maximum(state["top"], top)
                state["top"] = top
                if step == steps - 1:
                    top_scr[pair, half] = top

            for pair in range(pairs):
                for half in range(2):
                    for step in range(steps):
                        units.append(functools.partial(score_block, pair, half, step))
            return units[:early], units[early:]

        def back(value_scr, score_scr, top_scr):
            sums = [None] * (2 * pairs)

            def add_block(pair, step, head):
                where = slice(head * half_rows, (head + 1) * half_rows)
                parts = []
                for half in range(2):
                    start, stop = span(step, half)
                    part = jnp.exp2(
                        score_scr[pair, half, step, start:stop, where]
                        - top_scr[pair, half][:, where]
                    )
                    part = [part.astype(jnp.bfloat16)]
                    if start > 0:
                        part = [jnp.zeros((start, half_rows), jnp.bfloat16)] + part
                    if stop < rows:
                        part = part + [jnp.zeros((rows - stop, half_rows), jnp.bfloat16)]
                    parts.append(jnp.concatenate(part, 0) if len(part) > 1 else part[0])
                weights = jnp.concatenate(parts, 1)
                first = pair * LANES + head * head_size
                left = jnp.concatenate(
                    [
                        value_scr[core + step, first : first + head_size, :],
                        jnp.ones((16, rows), jnp.bfloat16),
                    ],
                    0,
                )
                add = jnp.dot(left, weights, preferred_element_type=jnp.float32)
                place = 2 * pair + head
                sums[place] = add if sums[place] is None else sums[place] + add

            def write(pair):
                query_valid = (
                    lax.broadcasted_iota(jnp.int32, (1, rows), 1) >= valid_first - query_first
                )
                outs = []
                for head in range(2):
                    result = sums[2 * pair + head]
                    total = result[head_size : head_size + 1]
                    factor = jnp.where(query_valid, 1.0 / total, 0.0)
                    outs.append(result[:head_size] * factor)
                first = jnp.maximum(index - 1, 0) * chunk + pair * LANES
                where = pl.ds(pl.multiple_of(first, LANES), LANES)
                attended_scr[:, where] = jnp.concatenate(outs, 0).T.astype(jnp.bfloat16)

            units = []
            for pair in range(pairs):
                for head in range(2):
                    for step in range(steps):
                        units.append(functools.partial(add_block, pair, step, head))
                units.append(functools.partial(write, pair))
            return units

        def interleave(first, second):
            done = 0
            for number, unit in enumerate(first):
                unit()
                target = (number + 1) * len(second) // len(first)
                for other in second[done:target]:
                    other()
                done = target

        sets = [(value_scrs[n], score_scrs[n], top_scrs[n]) for n in range(2)]
        for parity in range(2):

            @pl.when((index < chunks) & (index % 2 == parity))
            def _():
                early, late = front(*sets[parity])
                interleave(early, back(*sets[1 - parity]))
                interleave(late, [])

        @pl.when(index == chunks)
        def _():
            for unit in back(*sets[(chunks - 1) % 2]):
                unit()
            for copy in copies:
                copy.wait()
            update = jnp.dot(attended_scr[...], wo_scr[...], preferred_element_type=jnp.float32)
            hidden = (rows_ref[...].astype(jnp.float32) + update).astype(jnp.bfloat16)
            hidden_ref[...] = hidden
            branch_ref[...] = jnp.dot(
                hidden, down_scr[...], preferred_element_type=jnp.float32
            ).astype(jnp.bfloat16)

    ahead = lambda g: jnp.minimum(g, chunks - 1)
    block = pl.BlockSpec((rows, chunk), lambda g, *_: (0, ahead(g)))
    key_spec = lambda count: pl.BlockSpec((count, rows, chunk), lambda g, *_: (0, 0, ahead(g)))
    value_spec = lambda count: pl.BlockSpec((count, chunk, rows), lambda g, *_: (0, ahead(g), 0))
    weight_spec = lambda part: pl.BlockSpec(
        (width, chunk), lambda g, *_: (0, part * chunks + ahead(g))
    )
    in_specs = [pl.BlockSpec((rows, width), lambda g, *_: (0, 0)) for _ in raw]
    operands = list(raw)
    for keys, values in ready:
        in_specs += [key_spec(2), value_spec(2)]
        operands += [keys, values]
    whole = lambda shape: pl.BlockSpec(shape, lambda g, *_: (0, 0))
    if home:
        in_specs += [whole((rows, width)), block]
        operands += own
    else:
        in_specs.append(weight_spec(0))
        operands.append(weight)
    in_specs += [weight_spec(1), weight_spec(2)] + [pl.BlockSpec(memory_space=pl.ANY)] * 2
    operands += [weight, weight, output_proj, mixer_down]
    inner = mixer_down.shape[1]
    out_shape = [
        jax.ShapeDtypeStruct((rows, width), jnp.bfloat16),
        jax.ShapeDtypeStruct((rows, inner), jnp.bfloat16),
    ]
    out_specs = [whole((rows, width)), whole((rows, inner))]
    if keep:
        out_shape += [
            jax.ShapeDtypeStruct((keep, rows, width), jnp.bfloat16),
            jax.ShapeDtypeStruct((keep, width, rows), jnp.bfloat16),
        ]
        out_specs += [key_spec(keep), value_spec(keep)]
    twice = lambda shape, dtype: [pltpu.VMEM(shape, dtype)] * 2
    return pl.pallas_call(
        body,
        out_shape=tuple(out_shape),
        grid_spec=pltpu.PrefetchScalarGridSpec(
            num_scalar_prefetch=3,
            grid=(chunks + 1,),
            in_specs=in_specs,
            out_specs=tuple(out_specs),
            scratch_shapes=[
                pltpu.VMEM((slot_count, rows, chunk), jnp.bfloat16),
                pltpu.VMEM((rows, LANES), jnp.int32),
                pltpu.VMEM((rows, chunk), jnp.bfloat16),
            ]
            + twice((slot_count, chunk, rows), jnp.bfloat16)
            + twice((pairs, 2, steps, rows, cols), jnp.float32)
            + twice((pairs, 2, 1, cols), jnp.float32)
            + [
                pltpu.VMEM((rows, width), jnp.bfloat16),
                pltpu.VMEM(output_proj.shape, jnp.bfloat16),
                pltpu.VMEM(mixer_down.shape, jnp.bfloat16),
                pltpu.SemaphoreType.DMA((2,)),
            ],
        ),
        cost_estimate=pl.CostEstimate(
            flops=(8 * steps * rows + 4 * raw_count * width) * rows * width,
            bytes_accessed=4 * width * width + 4 * steps * rows * width,
            transcendentals=steps * rows * rows * HEADS,
        ),
        name="attend",
    )(place, head_window, lengths, *operands)


def mix(place, own_group, series_mix, weight, hidden, branches):
    rows, width = hidden[0].shape
    groups = len(branches[0])

    def body(place_ref, group_ref, mix_ref, weight_ref, *refs):
        hidden_refs = refs[:2]
        branch_refs = refs[2 : 2 + 2 * groups]
        out_ref = refs[-1]
        own = group_ref[0]
        chip = (place_ref[0] // 2) % 2
        series = [chip, 1 - chip]
        for which in range(2):
            row = 2 * own + series[which]
            total = None
            for number, branch_ref in enumerate(branch_refs):
                kind, shift = number // groups, number % groups
                group = (own + shift) % groups
                term = mix_ref[row, 2 * group + series[kind]] * branch_ref[...].astype(jnp.float32)
                total = term if total is None else total + term
            update = jnp.dot(
                total.astype(jnp.bfloat16), weight_ref[...], preferred_element_type=jnp.float32
            )
            out_ref[series[which]] = (
                hidden_refs[which][...].astype(jnp.float32) + update
            ).astype(out_ref.dtype)

    small = pl.BlockSpec(memory_space=pltpu.SMEM)
    large = pl.BlockSpec(memory_space=pltpu.VMEM)
    return pl.pallas_call(
        body,
        out_shape=jax.ShapeDtypeStruct((2, rows, width), jnp.bfloat16),
        in_specs=[small] * 3 + [large] * (3 + 2 * groups),
        out_specs=large,
        cost_estimate=pl.CostEstimate(
            flops=4 * rows * weight.size, bytes_accessed=2 * weight.size, transcendentals=0
        ),
        name="mix",
    )(place, own_group, series_mix, weight, *hidden, *branches[0], *branches[1])


def on_device(
    history, lengths, head_window, input_proj, output_proj, mixer_down, mixer_up, series_mix
):
    local_series, rows, width = history.shape
    devices = lax.axis_size("tm")
    groups = lax.axis_size("series")
    assert local_series == 2 and devices % 4 == 0 and WINDOW == 2 * rows
    position = lax.axis_index("tm")
    chip = (position // 2) % 2
    chip_swap, core_swap, near_route, far_route, far_cross = routes(devices)

    def move(block, route):
        return lax.ppermute(block, "tm", route)

    def part(array, index):
        return lax.dynamic_index_in_dim(array, index, 0, keepdims=False)

    mine = part(history, chip)
    other = part(history, 1 - chip)
    away = move(other, chip_swap)
    near = move(mine, near_route)
    mine_beside = move(mine, core_swap)
    scale = (width // HEADS) ** (-0.5) * math.log2(math.e)
    place = position.astype(jnp.int32)[None]
    attention = functools.partial(
        attend, place, head_window, lengths, input_proj, output_proj, mixer_down, scale
    )

    home_queries, *home_ready = project(mine, mine_beside, input_proj, scale)
    away, home_queries = lax.optimization_barrier((away, home_queries))
    away_beside = move(away, core_swap)
    near, away_beside = lax.optimization_barrier((near, away_beside))
    near_beside = move(near, core_swap)
    far = move(away, far_route)
    far_beside = move(away, far_cross)
    away_hidden, away_branch, *away_ready = attention(
        False,
        [(0, [away, away_beside]), (1, [near, near_beside])],
        [(-1, home_ready)],
        keep=2,
    )
    away_hidden, far, far_beside = lax.optimization_barrier((away_hidden, far, far_beside))

    def down(hidden):
        return jnp.dot(hidden, mixer_down, preferred_element_type=jnp.float32).astype(jnp.bfloat16)

    other_hidden = move(away_hidden, chip_swap)
    other_branches = []
    for shift in range(1, groups):
        route = [
            (i * groups + (g + shift) % groups, home * groups + g)
            for g in range(groups)
            for i, home in chip_swap
        ]
        other_branches.append(lax.ppermute(away_branch, ("tm", "series"), route))

    mine_hidden, mine_branch = attention(
        True,
        [(-1, [far, far_beside])],
        [(0, home_ready), (1, away_ready)],
        own=[mine, home_queries],
    )
    mine_branches = [mine_branch]
    for shift in range(1, groups):
        route = [((g + shift) % groups, g) for g in range(groups)]
        mine_branches.append(lax.ppermute(mine_branch, "series", route))
    other_hidden, mine_branch = lax.optimization_barrier((other_hidden, mine_branch))
    other_branches = [down(other_hidden)] + other_branches

    own_group = lax.axis_index("series")
    return mix(
        place,
        own_group.astype(jnp.int32)[None],
        series_mix.astype(jnp.float32),
        mixer_up,
        (mine_hidden, other_hidden),
        (mine_branches, other_branches),
    )


def solution(mesh):
    in_specs = (P("series", "tm", None), P("series"), P(), P(), P(), P(), P(), P())
    out_specs = P("series", "tm", None)
    return jax.shard_map(
        on_device, mesh=mesh, in_specs=in_specs, out_specs=out_specs, check_vma=False
    )
```

```python
import functools
import math

import jax
import jax.numpy as jnp
from jax import lax
from jax.experimental import pallas as pl
from jax.experimental.pallas import tpu as pltpu
from jax.sharding import PartitionSpec as P

HEADS = 16
WINDOW = 512
LANES = 128
MASKED = -1e30


def routes(count):
    place = lambda quad, chip, core: 4 * quad + 2 * chip + core
    last = count // 4 - 1
    chip_swap = [(i, i ^ 2) for i in range(count)]
    core_swap = [(i, i ^ 1) for i in range(count)]
    near, far, far_cross = [], [], []
    for i in range(count):
        quad, chip, core = i // 4, (i // 2) % 2, i % 2
        down = quad - 1 if quad > 0 else None
        up = quad + 1 if quad < last else None
        near_quad, far_quad = (down, up) if chip == 0 else (up, down)
        if near_quad is not None:
            near.append((i, place(near_quad, chip, core)))
        if far_quad is not None:
            far.append((i, place(far_quad, chip, core)))
            if core != chip:
                far_cross.append((i, place(far_quad, chip, chip)))
    return chip_swap, core_swap, near, far, far_cross


def project(first, beside, weight, scale):
    rows, width = first.shape
    chunk = min(256, width)
    steps = width // chunk

    def body(first_ref, beside_ref, wq_ref, wk_ref, wv_ref, q_ref, k_ref, v_ref):
        def dot(block, ref):
            return jnp.dot(block[...], ref[...], preferred_element_type=jnp.float32)

        q_ref[...] = (dot(first_ref, wq_ref) * scale).astype(jnp.bfloat16)
        for index, block in enumerate((first_ref, beside_ref)):
            k_ref[index] = dot(block, wk_ref).astype(jnp.bfloat16)
            v_ref[index] = dot(block, wv_ref).astype(jnp.bfloat16).T

    whole = pl.BlockSpec((rows, width), lambda g: (0, 0))
    weights = [
        pl.BlockSpec((width, chunk), lambda g, part=part: (0, part * steps + g))
        for part in range(3)
    ]
    return pl.pallas_call(
        body,
        out_shape=(
            jax.ShapeDtypeStruct((rows, width), jnp.bfloat16),
            jax.ShapeDtypeStruct((2, rows, width), jnp.bfloat16),
            jax.ShapeDtypeStruct((2, width, rows), jnp.bfloat16),
        ),
        grid=(steps,),
        in_specs=[whole, whole] + weights,
        out_specs=(
            pl.BlockSpec((rows, chunk), lambda g: (0, g)),
            pl.BlockSpec((2, rows, chunk), lambda g: (0, 0, g)),
            pl.BlockSpec((2, chunk, rows), lambda g: (0, g, 0)),
        ),
        cost_estimate=pl.CostEstimate(
            flops=10 * rows * width * width, bytes_accessed=6 * width * width, transcendentals=0
        ),
        name="project",
    )(first, beside, weight, weight, weight)


def attend(
    place, head_window, lengths, weight, output_proj, mixer_down, scale, home, raw, ready,
    own=None, keep=0,
):
    raw_sides = [side for side, _ in raw]
    ready_sides = [side for side, _ in ready]
    raw = [block for _, blocks in raw for block in blocks]
    ready = [arrays for _, arrays in ready]
    rows, width = raw[0].shape
    devices = lax.axis_size("tm")
    head_size = width // HEADS
    chunk = 2 * LANES
    chunks = width // chunk
    pairs = chunk // LANES
    reach = WINDOW // rows
    steps = 2 * reach + 1
    slot_count = steps + 1
    half_rows = rows // 2
    cols = 2 * half_rows
    raw_count, ready_count = len(raw), len(ready)

    def span(step, half):
        if step == 0 and half == 1:
            return half_rows, rows
        if step == steps - 1 and half == 0:
            return 0, half_rows
        return 0, rows

    def body(place_ref, window_ref, length_ref, *refs):
        refs = list(refs)
        take = lambda count: [refs.pop(0) for _ in range(count)]
        raw_refs = take(raw_count)
        ready_refs = take(2 * ready_count)
        rows_ref, query_ref = take(2) if home else (raw_refs[0], None)
        wq_ref = None if home else take(1)[0]
        wk_ref, wv_ref, wo_hbm, down_hbm = take(4)
        hidden_ref, branch_ref = take(2)
        keep_refs = take(2) if keep else None
        key_scr, row_scr, query_scr = take(3)
        value_scrs, score_scrs, top_scrs = take(2), take(2), take(2)
        attended_scr, update_scr, wo_scr, down_scr, copy_sems = take(5)
        index = pl.program_id(0)
        position = place_ref[0]
        core = position % 2
        chip = (position // 2) % 2
        patches = rows * devices
        valid_first = patches - length_ref[chip]
        query_chip = chip if home else 1 - chip
        query_first = (position - 2 * chip + 2 * query_chip) * rows

        def slot_of(side, beside):
            offset = core if not beside else 1 - core
            return 2 + 2 * side * (1 - 2 * chip) + offset

        copies = [
            pltpu.make_async_copy(wo_hbm, wo_scr, copy_sems.at[0]),
            pltpu.make_async_copy(down_hbm, down_scr, copy_sems.at[1]),
        ]

        @pl.when(index == 0)
        def _():
            for copy in copies:
                copy.start()
            row_scr[...] = lax.broadcasted_iota(jnp.int32, (rows, LANES), 0)

        def front(value_scr, score_scr, top_scr):
            units = []
            state = {}

            def ready_blocks():
                for number in range(ready_count):
                    for which in range(2):
                        slot = slot_of(ready_sides[number], which)
                        key_scr[slot] = ready_refs[2 * number][which]
                        value_scr[slot] = ready_refs[2 * number + 1][which]

            units.append(ready_blocks)

            def project_queries():
                both = jnp.dot(raw_refs[0][...], wq_ref[...], preferred_element_type=jnp.float32)
                query_scr[...] = (both * scale).astype(jnp.bfloat16)

            if query_ref is None:
                units.append(project_queries)

            def project_keys(number):
                slot = slot_of(raw_sides[number // 2], number % 2)
                keys = jnp.dot(
                    raw_refs[number][...], wk_ref[...], preferred_element_type=jnp.float32
                ).astype(jnp.bfloat16)
                key_scr[slot] = keys
                if number < keep:
                    keep_refs[0][number] = keys

            def project_values(number):
                slot = slot_of(raw_sides[number // 2], number % 2)
                values = jnp.dot(
                    raw_refs[number][...], wv_ref[...], preferred_element_type=jnp.float32
                ).astype(jnp.bfloat16).T
                value_scr[slot] = values
                if number < keep:
                    keep_refs[1][number] = values

            for project in (project_keys, project_values):
                for number in range(raw_count):
                    units.append(functools.partial(project, number))
            early = len(units)

            def bounds(pair, half):
                column = lax.broadcasted_iota(jnp.int32, (1, cols), 1)
                second = column >= half_rows
                head = 2 * (pairs * index + pair)
                window = jnp.where(second, window_ref[head + 1], window_ref[head])
                lane = lax.broadcasted_iota(jnp.int32, (half_rows, LANES), 1)
                local = jnp.where(second, column - half_rows, column) + half * half_rows
                lowest = jnp.maximum(local - window, valid_first - query_first)
                highest = jnp.minimum(local + window, patches - 1 - query_first)
                where = slice(half * half_rows, (half + 1) * half_rows)
                source = query_scr if query_ref is None else query_ref
                part = source[where, pair * LANES : (pair + 1) * LANES]
                zero = jnp.zeros_like(part)
                right = jnp.concatenate(
                    [
                        jnp.where(lane < head_size, part, zero),
                        jnp.where(lane < head_size, zero, part),
                    ],
                    0,
                )
                return right, lowest, highest

            def score_block(pair, half, step):
                if step == 0:
                    state["bounds"] = bounds(pair, half)
                right, lowest, highest = state["bounds"]
                start, stop = span(step, half)
                first = (step - reach) * rows
                scores = lax.dot_general(
                    key_scr[core + step, start:stop, pair * LANES : (pair + 1) * LANES],
                    right,
                    (((1,), (1,)), ((), ())),
                    preferred_element_type=jnp.float32,
                )
                key_row = row_scr[start:stop, :]
                key_row = jnp.concatenate([key_row] * (cols // LANES), 1)
                allowed = None
                if step <= reach:
                    allowed = key_row >= lowest - first
                if step >= reach:
                    upper = key_row <= highest - first
                    allowed = upper if allowed is None else allowed & upper
                scores = jnp.where(allowed, scores, MASKED)
                score_scr[pair, half, step, start:stop, :] = scores
                top = jnp.max(scores, axis=0, keepdims=True)
                if step > 0:
                    top = jnp.maximum(state["top"], top)
                state["top"] = top
                if step == steps - 1:
                    top_scr[pair, half] = top

            for pair in range(pairs):
                for half in range(2):
                    for step in range(steps):
                        units.append(functools.partial(score_block, pair, half, step))
            return units[:early], units[early:]

        def back(value_scr, score_scr, top_scr, last=False):
            sums = [None] * (2 * pairs)

            def add_block(pair, step, head):
                where = slice(head * half_rows, (head + 1) * half_rows)
                parts = []
                for half in range(2):
                    start, stop = span(step, half)
                    part = jnp.exp2(
                        score_scr[pair, half, step, start:stop, where]
                        - top_scr[pair, half][:, where]
                    )
                    part = [part.astype(jnp.bfloat16)]
                    if start > 0:
                        part = [jnp.zeros((start, half_rows), jnp.bfloat16)] + part
                    if stop < rows:
                        part = part + [jnp.zeros((rows - stop, half_rows), jnp.bfloat16)]
                    parts.append(jnp.concatenate(part, 0) if len(part) > 1 else part[0])
                weights = jnp.concatenate(parts, 1)
                first = pair * LANES + head * head_size
                left = jnp.concatenate(
                    [
                        value_scr[core + step, first : first + head_size, :],
                        jnp.ones((16, rows), jnp.bfloat16),
                    ],
                    0,
                )
                add = jnp.dot(left, weights, preferred_element_type=jnp.float32)
                place = 2 * pair + head
                sums[place] = add if sums[place] is None else sums[place] + add

            def write(pair):
                query_valid = (
                    lax.broadcasted_iota(jnp.int32, (1, rows), 1) >= valid_first - query_first
                )
                outs = []
                for head in range(2):
                    result = sums[2 * pair + head]
                    total = result[head_size : head_size + 1]
                    factor = jnp.where(query_valid, 1.0 / total, 0.0)
                    outs.append(result[:head_size] * factor)
                if last:
                    where = slice(width - chunk + pair * LANES, width - chunk + (pair + 1) * LANES)
                else:
                    first = (index - 1) * chunk + pair * LANES
                    where = pl.ds(pl.multiple_of(first, LANES), LANES)
                attended_scr[:, where] = jnp.concatenate(outs, 0).T.astype(jnp.bfloat16)

            units = []
            for pair in range(pairs):
                for head in range(2):
                    for step in range(steps):
                        units.append(functools.partial(add_block, pair, step, head))
                units.append(functools.partial(write, pair))
            return units

        def interleave(first, second):
            done = 0
            for number, unit in enumerate(first):
                unit()
                target = (number + 1) * len(second) // len(first)
                for other in second[done:target]:
                    other()
                done = target

        sets = [(value_scrs[n], score_scrs[n], top_scrs[n]) for n in range(2)]

        @pl.when(index == 0)
        def _():
            early, late = front(*sets[0])
            interleave(early + late, [])

        for parity in range(2):

            @pl.when((index > 0) & (index < chunks) & (index % 2 == parity))
            def _():
                early, late = front(*sets[parity])
                interleave(early, back(*sets[1 - parity]))
                interleave(late, [])

        @pl.when(index == chunks)
        def _():
            for copy in copies:
                copy.wait()
            before = width - chunk

            def update_block(column):
                where = slice(column * chunk, (column + 1) * chunk)
                update_scr[:, where] = jnp.dot(
                    attended_scr[:, :before],
                    wo_scr[:before, where],
                    preferred_element_type=jnp.float32,
                )

            updates = [functools.partial(update_block, column) for column in range(chunks)]
            interleave(updates, back(*sets[(chunks - 1) % 2], last=True))
            update = update_scr[...] + jnp.dot(
                attended_scr[:, before:], wo_scr[before:, :], preferred_element_type=jnp.float32
            )
            hidden = (rows_ref[...].astype(jnp.float32) + update).astype(jnp.bfloat16)
            hidden_ref[...] = hidden
            branch_ref[...] = jnp.dot(
                hidden, down_scr[...], preferred_element_type=jnp.float32
            ).astype(jnp.bfloat16)

    ahead = lambda g: jnp.minimum(g, chunks - 1)
    block = pl.BlockSpec((rows, chunk), lambda g, *_: (0, ahead(g)))
    key_spec = lambda count: pl.BlockSpec((count, rows, chunk), lambda g, *_: (0, 0, ahead(g)))
    value_spec = lambda count: pl.BlockSpec((count, chunk, rows), lambda g, *_: (0, ahead(g), 0))
    weight_spec = lambda part: pl.BlockSpec(
        (width, chunk), lambda g, *_: (0, part * chunks + ahead(g))
    )
    in_specs = [pl.BlockSpec((rows, width), lambda g, *_: (0, 0)) for _ in raw]
    operands = list(raw)
    for keys, values in ready:
        in_specs += [key_spec(2), value_spec(2)]
        operands += [keys, values]
    whole = lambda shape: pl.BlockSpec(shape, lambda g, *_: (0, 0))
    if home:
        in_specs += [whole((rows, width)), block]
        operands += own
    else:
        in_specs.append(weight_spec(0))
        operands.append(weight)
    in_specs += [weight_spec(1), weight_spec(2)] + [pl.BlockSpec(memory_space=pl.ANY)] * 2
    operands += [weight, weight, output_proj, mixer_down]
    inner = mixer_down.shape[1]
    out_shape = [
        jax.ShapeDtypeStruct((rows, width), jnp.bfloat16),
        jax.ShapeDtypeStruct((rows, inner), jnp.bfloat16),
    ]
    out_specs = [whole((rows, width)), whole((rows, inner))]
    if keep:
        out_shape += [
            jax.ShapeDtypeStruct((keep, rows, width), jnp.bfloat16),
            jax.ShapeDtypeStruct((keep, width, rows), jnp.bfloat16),
        ]
        out_specs += [key_spec(keep), value_spec(keep)]
    twice = lambda shape, dtype: [pltpu.VMEM(shape, dtype)] * 2
    return pl.pallas_call(
        body,
        out_shape=tuple(out_shape),
        grid_spec=pltpu.PrefetchScalarGridSpec(
            num_scalar_prefetch=3,
            grid=(chunks + 1,),
            in_specs=in_specs,
            out_specs=tuple(out_specs),
            scratch_shapes=[
                pltpu.VMEM((slot_count, rows, chunk), jnp.bfloat16),
                pltpu.VMEM((rows, LANES), jnp.int32),
                pltpu.VMEM((rows, chunk), jnp.bfloat16),
            ]
            + twice((slot_count, chunk, rows), jnp.bfloat16)
            + twice((pairs, 2, steps, rows, cols), jnp.float32)
            + twice((pairs, 2, 1, cols), jnp.float32)
            + [
                pltpu.VMEM((rows, width), jnp.bfloat16),
                pltpu.VMEM((rows, width), jnp.float32),
                pltpu.VMEM(output_proj.shape, jnp.bfloat16),
                pltpu.VMEM(mixer_down.shape, jnp.bfloat16),
                pltpu.SemaphoreType.DMA((2,)),
            ],
        ),
        cost_estimate=pl.CostEstimate(
            flops=(8 * steps * rows + 4 * raw_count * width) * rows * width,
            bytes_accessed=4 * width * width + 4 * steps * rows * width,
            transcendentals=steps * rows * rows * HEADS,
        ),
        name="attend",
    )(place, head_window, lengths, *operands)


def on_device(
    history, lengths, head_window, input_proj, output_proj, mixer_down, mixer_up, series_mix
):
    local_series, rows, width = history.shape
    devices = lax.axis_size("tm")
    groups = lax.axis_size("series")
    assert local_series == 2 and devices % 4 == 0 and WINDOW == 2 * rows
    position = lax.axis_index("tm")
    chip = (position // 2) % 2
    chip_swap, core_swap, near_route, far_route, far_cross = routes(devices)

    def move(block, route):
        return lax.ppermute(block, "tm", route)

    def part(array, index):
        return lax.dynamic_index_in_dim(array, index, 0, keepdims=False)

    mine = part(history, chip)
    other = part(history, 1 - chip)
    away = move(other, chip_swap)
    near = move(mine, near_route)
    mine_beside = move(mine, core_swap)
    scale = (width // HEADS) ** (-0.5) * math.log2(math.e)
    place = position.astype(jnp.int32)[None]
    attention = functools.partial(
        attend, place, head_window, lengths, input_proj, output_proj, mixer_down, scale
    )

    home_queries, *home_ready = project(mine, mine_beside, input_proj, scale)
    away, home_queries = lax.optimization_barrier((away, home_queries))
    away_beside = move(away, core_swap)
    near, away_beside = lax.optimization_barrier((near, away_beside))
    near_beside = move(near, core_swap)
    far = move(away, far_route)
    far_beside = move(away, far_cross)
    away_hidden, away_branch, *away_ready = attention(
        False,
        [(0, [away, away_beside]), (1, [near, near_beside])],
        [(-1, home_ready)],
        keep=2,
    )
    away_hidden, far, far_beside = lax.optimization_barrier((away_hidden, far, far_beside))

    def down(hidden):
        return jnp.dot(hidden, mixer_down, preferred_element_type=jnp.float32).astype(jnp.bfloat16)

    other_hidden = move(away_hidden, chip_swap)
    other_branches = []
    for shift in range(1, groups):
        route = [
            (i * groups + (g + shift) % groups, home * groups + g)
            for g in range(groups)
            for i, home in chip_swap
        ]
        other_branches.append(lax.ppermute(away_branch, ("tm", "series"), route))

    mine_hidden, mine_branch = attention(
        True,
        [(-1, [far, far_beside])],
        [(0, home_ready), (1, away_ready)],
        own=[mine, home_queries],
    )
    mine_branches = [mine_branch]
    for shift in range(1, groups):
        route = [((g + shift) % groups, g) for g in range(groups)]
        mine_branches.append(lax.ppermute(mine_branch, "series", route))
    other_hidden, mine_branch = lax.optimization_barrier((other_hidden, mine_branch))
    other_branches = [down(other_hidden)] + other_branches

    own_group = lax.axis_index("series")
    hidden = jnp.where(
        chip == 0,
        jnp.stack([mine_hidden, other_hidden]),
        jnp.stack([other_hidden, mine_hidden]),
    )
    rows_of_mix = lax.dynamic_slice_in_dim(series_mix.astype(jnp.float32), 2 * own_group, 2, 0)
    combined = 0.0
    for branches, series in ((mine_branches, chip), (other_branches, 1 - chip)):
        for shift, branch in enumerate(branches):
            group = (own_group + shift) % groups
            factor = lax.dynamic_slice_in_dim(rows_of_mix, 2 * group + series, 1, 1)
            combined += factor[:, :, None] * branch.astype(jnp.float32)[None]
    combined = lax.optimization_barrier(combined.astype(jnp.bfloat16))
    update = jnp.einsum("spc,cd->spd", combined, mixer_up, preferred_element_type=jnp.float32)
    return (hidden.astype(jnp.float32) + update).astype(jnp.bfloat16)


def solution(mesh):
    in_specs = (P("series", "tm", None), P("series"), P(), P(), P(), P(), P(), P())
    out_specs = P("series", "tm", None)
    return jax.shard_map(
        on_device, mesh=mesh, in_specs=in_specs, out_specs=out_specs, check_vma=False
    )
```

```python
import functools
import math

import jax
import jax.numpy as jnp
from jax import lax
from jax.experimental import pallas as pl
from jax.experimental.pallas import tpu as pltpu
from jax.sharding import PartitionSpec as P

HEADS = 16
WINDOW = 512
LANES = 128
MASKED = -1e30


def routes(count):
    place = lambda quad, chip, core: 4 * quad + 2 * chip + core
    last = count // 4 - 1
    chip_swap = [(i, i ^ 2) for i in range(count)]
    core_swap = [(i, i ^ 1) for i in range(count)]
    near, far, far_cross = [], [], []
    for i in range(count):
        quad, chip, core = i // 4, (i // 2) % 2, i % 2
        down = quad - 1 if quad > 0 else None
        up = quad + 1 if quad < last else None
        near_quad, far_quad = (down, up) if chip == 0 else (up, down)
        if near_quad is not None:
            near.append((i, place(near_quad, chip, core)))
        if far_quad is not None:
            far.append((i, place(far_quad, chip, core)))
            if core != chip:
                far_cross.append((i, place(far_quad, chip, chip)))
    return chip_swap, core_swap, near, far, far_cross


def project(first, beside, weight, scale):
    rows, width = first.shape
    chunk = min(256, width)
    steps = width // chunk

    def body(first_ref, beside_ref, wq_ref, wk_ref, wv_ref, q_ref, k_ref, v_ref):
        def dot(block, ref):
            return jnp.dot(block[...], ref[...], preferred_element_type=jnp.float32)

        q_ref[...] = (dot(first_ref, wq_ref) * scale).astype(jnp.bfloat16)
        for index, block in enumerate((first_ref, beside_ref)):
            k_ref[index] = dot(block, wk_ref).astype(jnp.bfloat16)
            v_ref[index] = dot(block, wv_ref).astype(jnp.bfloat16).T

    whole = pl.BlockSpec((rows, width), lambda g: (0, 0))
    weights = [
        pl.BlockSpec((width, chunk), lambda g, part=part: (0, part * steps + g))
        for part in range(3)
    ]
    return pl.pallas_call(
        body,
        out_shape=(
            jax.ShapeDtypeStruct((rows, width), jnp.bfloat16),
            jax.ShapeDtypeStruct((2, rows, width), jnp.bfloat16),
            jax.ShapeDtypeStruct((2, width, rows), jnp.bfloat16),
        ),
        grid=(steps,),
        in_specs=[whole, whole] + weights,
        out_specs=(
            pl.BlockSpec((rows, chunk), lambda g: (0, g)),
            pl.BlockSpec((2, rows, chunk), lambda g: (0, 0, g)),
            pl.BlockSpec((2, chunk, rows), lambda g: (0, g, 0)),
        ),
        cost_estimate=pl.CostEstimate(
            flops=10 * rows * width * width, bytes_accessed=6 * width * width, transcendentals=0
        ),
        name="project",
    )(first, beside, weight, weight, weight)


def attend(
    place, head_window, lengths, weight, output_proj, mixer_down, scale, home, raw, ready,
    own=None, keep=0,
):
    raw_sides = [side for side, _ in raw]
    ready_sides = [side for side, _ in ready]
    raw = [block for _, blocks in raw for block in blocks]
    ready = [arrays for _, arrays in ready]
    rows, width = raw[0].shape
    devices = lax.axis_size("tm")
    head_size = width // HEADS
    chunk = 2 * LANES
    chunks = width // chunk
    pairs = chunk // LANES
    reach = WINDOW // rows
    steps = 2 * reach + 1
    slot_count = steps + 1
    half_rows = rows // 2
    cols = 2 * half_rows
    raw_count, ready_count = len(raw), len(ready)

    def span(step, half):
        if step == 0 and half == 1:
            return half_rows, rows
        if step == steps - 1 and half == 0:
            return 0, half_rows
        return 0, rows

    def body(place_ref, window_ref, length_ref, *refs):
        refs = list(refs)
        take = lambda count: [refs.pop(0) for _ in range(count)]
        raw_refs = take(raw_count)
        ready_refs = take(2 * ready_count)
        rows_hbm, query_ref = take(2) if home else (None, None)
        wq_ref = None if home else take(1)[0]
        wk_ref, wv_ref, wo_hbm, down_hbm = take(4)
        hidden_ref, branch_ref = take(2)
        keep_refs = take(2) if keep else None
        key_scr, row_scr, query_scr = take(3)
        value_scrs, score_scrs, top_scrs = take(2), take(2), take(2)
        attended_scr, update_scr, wo_scr, down_scr, copy_sems = take(5)
        rows_ref = take(1)[0] if home else raw_refs[0]
        index = pl.program_id(0)
        position = place_ref[0]
        core = position % 2
        chip = (position // 2) % 2
        patches = rows * devices
        valid_first = patches - length_ref[chip]
        query_chip = chip if home else 1 - chip
        query_first = (position - 2 * chip + 2 * query_chip) * rows

        def slot_of(side, beside):
            offset = core if not beside else 1 - core
            return 2 + 2 * side * (1 - 2 * chip) + offset

        copies = [
            pltpu.make_async_copy(wo_hbm, wo_scr, copy_sems.at[0]),
            pltpu.make_async_copy(down_hbm, down_scr, copy_sems.at[1]),
        ]
        if home:
            copies.append(pltpu.make_async_copy(rows_hbm, rows_ref, copy_sems.at[2]))

        @pl.when(index == 0)
        def _():
            for copy in copies:
                copy.start()
            row_scr[...] = lax.broadcasted_iota(jnp.int32, (rows, LANES), 0)

        def front(value_scr, score_scr, top_scr):
            units = []
            state = {}

            def ready_blocks():
                for number in range(ready_count):
                    for which in range(2):
                        slot = slot_of(ready_sides[number], which)
                        key_scr[slot] = ready_refs[2 * number][which]
                        value_scr[slot] = ready_refs[2 * number + 1][which]

            units.append(ready_blocks)

            def project_queries():
                both = jnp.dot(raw_refs[0][...], wq_ref[...], preferred_element_type=jnp.float32)
                query_scr[...] = (both * scale).astype(jnp.bfloat16)

            if query_ref is None:
                units.append(project_queries)

            def project_keys(number):
                slot = slot_of(raw_sides[number // 2], number % 2)
                keys = jnp.dot(
                    raw_refs[number][...], wk_ref[...], preferred_element_type=jnp.float32
                ).astype(jnp.bfloat16)
                key_scr[slot] = keys
                if number < keep:
                    keep_refs[0][number] = keys

            def project_values(number):
                slot = slot_of(raw_sides[number // 2], number % 2)
                values = jnp.dot(
                    raw_refs[number][...], wv_ref[...], preferred_element_type=jnp.float32
                ).astype(jnp.bfloat16).T
                value_scr[slot] = values
                if number < keep:
                    keep_refs[1][number] = values

            for project in (project_keys, project_values):
                for number in range(raw_count):
                    units.append(functools.partial(project, number))
            early = len(units)

            def bounds(pair, half):
                column = lax.broadcasted_iota(jnp.int32, (1, cols), 1)
                second = column >= half_rows
                head = 2 * (pairs * index + pair)
                window = jnp.where(second, window_ref[head + 1], window_ref[head])
                lane = lax.broadcasted_iota(jnp.int32, (half_rows, LANES), 1)
                local = jnp.where(second, column - half_rows, column) + half * half_rows
                lowest = jnp.maximum(local - window, valid_first - query_first)
                highest = jnp.minimum(local + window, patches - 1 - query_first)
                where = slice(half * half_rows, (half + 1) * half_rows)
                source = query_scr if query_ref is None else query_ref
                part = source[where, pair * LANES : (pair + 1) * LANES]
                zero = jnp.zeros_like(part)
                right = jnp.concatenate(
                    [
                        jnp.where(lane < head_size, part, zero),
                        jnp.where(lane < head_size, zero, part),
                    ],
                    0,
                )
                return right, lowest, highest

            def score_block(pair, half, step):
                if step == 0:
                    state["bounds"] = bounds(pair, half)
                right, lowest, highest = state["bounds"]
                start, stop = span(step, half)
                first = (step - reach) * rows
                scores = lax.dot_general(
                    key_scr[core + step, start:stop, pair * LANES : (pair + 1) * LANES],
                    right,
                    (((1,), (1,)), ((), ())),
                    preferred_element_type=jnp.float32,
                )
                key_row = row_scr[start:stop, :]
                key_row = jnp.concatenate([key_row] * (cols // LANES), 1)
                if step < reach:
                    allowed = key_row >= lowest - first
                elif step > reach:
                    allowed = key_row <= highest - first
                else:
                    above = (key_row - (lowest - first)).astype(jnp.uint32)
                    allowed = above <= (highest - lowest).astype(jnp.uint32)
                scores = jnp.where(allowed, scores, MASKED)
                score_scr[pair, half, step, start:stop, :] = scores
                top = jnp.max(scores, axis=0, keepdims=True)
                if step > 0:
                    top = jnp.maximum(state["top"], top)
                state["top"] = top
                if step == steps - 1:
                    top_scr[pair, half] = top

            for pair in range(pairs):
                for half in range(2):
                    for step in range(steps):
                        units.append(functools.partial(score_block, pair, half, step))
            return units[:early], units[early:]

        def back(value_scr, score_scr, top_scr, last=False):
            sums = [None] * (2 * pairs)

            def add_block(pair, step, head):
                where = slice(head * half_rows, (head + 1) * half_rows)
                parts = []
                for half in range(2):
                    start, stop = span(step, half)
                    part = jnp.exp2(
                        score_scr[pair, half, step, start:stop, where]
                        - top_scr[pair, half][:, where]
                    )
                    part = [part.astype(jnp.bfloat16)]
                    if start > 0:
                        part = [jnp.zeros((start, half_rows), jnp.bfloat16)] + part
                    if stop < rows:
                        part = part + [jnp.zeros((rows - stop, half_rows), jnp.bfloat16)]
                    parts.append(jnp.concatenate(part, 0) if len(part) > 1 else part[0])
                weights = jnp.concatenate(parts, 1)
                first = pair * LANES + head * head_size
                left = jnp.concatenate(
                    [
                        value_scr[core + step, first : first + head_size, :],
                        jnp.ones((16, rows), jnp.bfloat16),
                    ],
                    0,
                )
                add = jnp.dot(left, weights, preferred_element_type=jnp.float32)
                place = 2 * pair + head
                sums[place] = add if sums[place] is None else sums[place] + add

            def write(pair):
                query_valid = (
                    lax.broadcasted_iota(jnp.int32, (1, rows), 1) >= valid_first - query_first
                )
                outs = []
                for head in range(2):
                    result = sums[2 * pair + head]
                    total = result[head_size : head_size + 1]
                    factor = jnp.where(query_valid, 1.0 / total, 0.0)
                    outs.append(result[:head_size] * factor)
                if last:
                    where = slice(width - chunk + pair * LANES, width - chunk + (pair + 1) * LANES)
                else:
                    first = (index - 1) * chunk + pair * LANES
                    where = pl.ds(pl.multiple_of(first, LANES), LANES)
                attended_scr[:, where] = jnp.concatenate(outs, 0).T.astype(jnp.bfloat16)

            units = []
            for pair in range(pairs):
                for head in range(2):
                    for step in range(steps):
                        units.append(functools.partial(add_block, pair, step, head))
                units.append(functools.partial(write, pair))
            return units

        def interleave(first, second):
            done = 0
            for number, unit in enumerate(first):
                unit()
                target = (number + 1) * len(second) // len(first)
                for other in second[done:target]:
                    other()
                done = target

        sets = [(value_scrs[n], score_scrs[n], top_scrs[n]) for n in range(2)]

        @pl.when(index == 0)
        def _():
            early, late = front(*sets[0])
            interleave(early + late, [])

        for parity in range(2):

            @pl.when((index > 0) & (index < chunks) & (index % 2 == parity))
            def _():
                early, late = front(*sets[parity])
                interleave(early, back(*sets[1 - parity]))
                interleave(late, [])

        @pl.when(index == chunks)
        def _():
            for copy in copies:
                copy.wait()
            before = width - chunk

            def update_block(column):
                where = slice(column * chunk, (column + 1) * chunk)
                update_scr[:, where] = jnp.dot(
                    attended_scr[:, :before],
                    wo_scr[:before, where],
                    preferred_element_type=jnp.float32,
                )

            updates = [functools.partial(update_block, column) for column in range(chunks)]
            interleave(updates, back(*sets[(chunks - 1) % 2], last=True))
            update = update_scr[...] + jnp.dot(
                attended_scr[:, before:], wo_scr[before:, :], preferred_element_type=jnp.float32
            )
            hidden = (rows_ref[...].astype(jnp.float32) + update).astype(jnp.bfloat16)
            hidden_ref[...] = hidden
            branch_ref[...] = jnp.dot(
                hidden, down_scr[...], preferred_element_type=jnp.float32
            ).astype(jnp.bfloat16)

    ahead = lambda g: jnp.minimum(g, chunks - 1)
    block = pl.BlockSpec((rows, chunk), lambda g, *_: (0, ahead(g)))
    key_spec = lambda count: pl.BlockSpec((count, rows, chunk), lambda g, *_: (0, 0, ahead(g)))
    value_spec = lambda count: pl.BlockSpec((count, chunk, rows), lambda g, *_: (0, ahead(g), 0))
    weight_spec = lambda part: pl.BlockSpec(
        (width, chunk), lambda g, *_: (0, part * chunks + ahead(g))
    )
    in_specs = [pl.BlockSpec((rows, width), lambda g, *_: (0, 0)) for _ in raw]
    operands = list(raw)
    for keys, values in ready:
        in_specs += [key_spec(2), value_spec(2)]
        operands += [keys, values]
    whole = lambda shape: pl.BlockSpec(shape, lambda g, *_: (0, 0))
    if home:
        in_specs += [pl.BlockSpec(memory_space=pl.ANY), block]
        operands += own
    else:
        in_specs.append(weight_spec(0))
        operands.append(weight)
    in_specs += [weight_spec(1), weight_spec(2)] + [pl.BlockSpec(memory_space=pl.ANY)] * 2
    operands += [weight, weight, output_proj, mixer_down]
    inner = mixer_down.shape[1]
    out_shape = [
        jax.ShapeDtypeStruct((rows, width), jnp.bfloat16),
        jax.ShapeDtypeStruct((rows, inner), jnp.bfloat16),
    ]
    out_specs = [whole((rows, width)), whole((rows, inner))]
    if keep:
        out_shape += [
            jax.ShapeDtypeStruct((keep, rows, width), jnp.bfloat16),
            jax.ShapeDtypeStruct((keep, width, rows), jnp.bfloat16),
        ]
        out_specs += [key_spec(keep), value_spec(keep)]
    twice = lambda shape, dtype: [pltpu.VMEM(shape, dtype)] * 2
    return pl.pallas_call(
        body,
        out_shape=tuple(out_shape),
        grid_spec=pltpu.PrefetchScalarGridSpec(
            num_scalar_prefetch=3,
            grid=(chunks + 1,),
            in_specs=in_specs,
            out_specs=tuple(out_specs),
            scratch_shapes=[
                pltpu.VMEM((slot_count, rows, chunk), jnp.bfloat16),
                pltpu.VMEM((rows, LANES), jnp.int32),
                pltpu.VMEM((rows, chunk), jnp.bfloat16),
            ]
            + twice((slot_count, chunk, rows), jnp.bfloat16)
            + twice((pairs, 2, steps, rows, cols), jnp.float32)
            + twice((pairs, 2, 1, cols), jnp.float32)
            + [
                pltpu.VMEM((rows, width), jnp.bfloat16),
                pltpu.VMEM((rows, width), jnp.float32),
                pltpu.VMEM(output_proj.shape, jnp.bfloat16),
                pltpu.VMEM(mixer_down.shape, jnp.bfloat16),
                pltpu.SemaphoreType.DMA((3,)),
            ]
            + [pltpu.VMEM((rows, width), jnp.bfloat16)] * home,
        ),
        cost_estimate=pl.CostEstimate(
            flops=(8 * steps * rows + 4 * raw_count * width) * rows * width,
            bytes_accessed=4 * width * width + 4 * steps * rows * width,
            transcendentals=steps * rows * rows * HEADS,
        ),
        name="attend",
    )(place, head_window, lengths, *operands)


def on_device(
    history, lengths, head_window, input_proj, output_proj, mixer_down, mixer_up, series_mix
):
    local_series, rows, width = history.shape
    devices = lax.axis_size("tm")
    groups = lax.axis_size("series")
    assert local_series == 2 and devices % 4 == 0 and WINDOW == 2 * rows
    position = lax.axis_index("tm")
    chip = (position // 2) % 2
    chip_swap, core_swap, near_route, far_route, far_cross = routes(devices)

    def move(block, route):
        return lax.ppermute(block, "tm", route)

    def part(array, index):
        return lax.dynamic_index_in_dim(array, index, 0, keepdims=False)

    mine = part(history, chip)
    other = part(history, 1 - chip)
    away = move(other, chip_swap)
    near = move(mine, near_route)
    mine_beside = move(mine, core_swap)
    scale = (width // HEADS) ** (-0.5) * math.log2(math.e)
    place = position.astype(jnp.int32)[None]
    attention = functools.partial(
        attend, place, head_window, lengths, input_proj, output_proj, mixer_down, scale
    )

    home_queries, *home_ready = project(mine, mine_beside, input_proj, scale)
    away, home_queries = lax.optimization_barrier((away, home_queries))
    away_beside = move(away, core_swap)
    near, away_beside = lax.optimization_barrier((near, away_beside))
    near_beside = move(near, core_swap)
    far = move(away, far_route)
    far_beside = move(away, far_cross)
    away_hidden, away_branch, *away_ready = attention(
        False,
        [(0, [away, away_beside]), (1, [near, near_beside])],
        [(-1, home_ready)],
        keep=2,
    )
    away_hidden, far, far_beside = lax.optimization_barrier((away_hidden, far, far_beside))

    def down(hidden):
        return jnp.dot(hidden, mixer_down, preferred_element_type=jnp.float32).astype(jnp.bfloat16)

    other_hidden = move(away_hidden, chip_swap)
    other_branches = []
    for shift in range(1, groups):
        route = [
            (i * groups + (g + shift) % groups, home * groups + g)
            for g in range(groups)
            for i, home in chip_swap
        ]
        other_branches.append(lax.ppermute(away_branch, ("tm", "series"), route))

    mine_hidden, mine_branch = attention(
        True,
        [(-1, [far, far_beside])],
        [(0, home_ready), (1, away_ready)],
        own=[mine, home_queries],
    )
    mine_branches = [mine_branch]
    for shift in range(1, groups):
        route = [((g + shift) % groups, g) for g in range(groups)]
        mine_branches.append(lax.ppermute(mine_branch, "series", route))
    other_hidden, mine_branch = lax.optimization_barrier((other_hidden, mine_branch))
    other_branches = [down(other_hidden)] + other_branches

    own_group = lax.axis_index("series")
    hidden = jnp.where(
        chip == 0,
        jnp.stack([mine_hidden, other_hidden]),
        jnp.stack([other_hidden, mine_hidden]),
    )
    rows_of_mix = lax.dynamic_slice_in_dim(series_mix.astype(jnp.float32), 2 * own_group, 2, 0)
    combined = 0.0
    for branches, series in ((mine_branches, chip), (other_branches, 1 - chip)):
        for shift, branch in enumerate(branches):
            group = (own_group + shift) % groups
            factor = lax.dynamic_slice_in_dim(rows_of_mix, 2 * group + series, 1, 1)
            combined += factor[:, :, None] * branch.astype(jnp.float32)[None]
    combined = lax.optimization_barrier(combined.astype(jnp.bfloat16))
    update = jnp.einsum("spc,cd->spd", combined, mixer_up, preferred_element_type=jnp.float32)
    return (hidden.astype(jnp.float32) + update).astype(jnp.bfloat16)


def solution(mesh):
    in_specs = (P("series", "tm", None), P("series"), P(), P(), P(), P(), P(), P())
    out_specs = P("series", "tm", None)
    return jax.shard_map(
        on_device, mesh=mesh, in_specs=in_specs, out_specs=out_specs, check_vma=False
    )
```
